32 devices in a mesh: dp: 1 (over z), sp2: 4 (over y), sp: 8 (over x, core).
Axes of the slice: x: 4, y: 4, z: 1, core: 2. Of those that a mesh axis runs over, the one named last changes fastest.
The devices are a block of a 4x4x8 slice.
Arguments:
- x: bfloat16 [8, 32, 192, 512], P('dp', 'sp', 'sp2')
- w_a: bfloat16 [4, 3, 3, 512, 512], replicated
- bn_a: float32 [4, 2, 512], replicated
- w_down: bfloat16 [3, 3, 512, 1024], replicated
- bn_down: float32 [2, 1024], replicated
- w_b: bfloat16 [1, 3, 3, 1024, 1024], replicated
- bn_b: float32 [1, 2, 1024], replicated
Outputs:
- output: bfloat16 [8, 16, 96, 1024], P('dp', 'sp', 'sp2')
All inputs are finite; a program needn't handle non-finite values.
Results may differ from the reference program's by a relative error of at most 0.0108284.
Values are sent between devices in bfloat16 or wider.
A program may use at most 768 MiB of HBM per device.

```python
import jax
import jax.numpy as jnp
from jax import lax

IMAGES = 8
IMG_HEIGHT = 32
IMG_WIDTH = 192
CHAN_A = 512
CHAN_B = 1024
LAYERS_A = 4
LAYERS_B = 1

CONV_DIMS = ("NHWC", "HWIO", "NHWC")
SAME_PADS = ((1, 1), (1, 1))
DOWN_PADS = ((0, 1), (0, 1))


def norm_pairs(pair_key, lead_shape, num_chan):
    gain_key, shift_key = jax.random.split(pair_key)
    gains = 1.0 + 0.3 * jax.random.normal(gain_key, lead_shape + (1, num_chan), jnp.float32)
    shifts = 0.5 * jax.random.normal(shift_key, lead_shape + (1, num_chan), jnp.float32)
    return jnp.concatenate([gains, shifts], axis=-2)


def conv_weights(w_key, lead_shape, chan_in, chan_out):
    raw_w = jax.random.normal(w_key, lead_shape + (3, 3, chan_in, chan_out), jnp.float32)
    return (raw_w * (9 * chan_in) ** -0.5).astype(jnp.bfloat16)


def setup_inputs(seed: int = 0, part: int = 0) -> dict:
    sub_keys = jax.random.split(jax.random.key(seed), 7)
    img_keys = jax.random.split(jax.random.fold_in(sub_keys[0], part), 3)
    noise = jax.random.normal(img_keys[0], (IMAGES, IMG_HEIGHT, IMG_WIDTH, CHAN_A), jnp.float32)
    row_amp = jax.random.normal(img_keys[1], (IMAGES, 1, 1, CHAN_A), jnp.float32)
    col_amp = jax.random.normal(img_keys[2], (IMAGES, 1, 1, CHAN_A), jnp.float32)
    row_pos = (2.0 * (jnp.arange(IMG_HEIGHT, dtype=jnp.float32) + 0.5) / IMG_HEIGHT - 1.0).reshape(1, IMG_HEIGHT, 1, 1)
    col_pos = (2.0 * (jnp.arange(IMG_WIDTH, dtype=jnp.float32) + 0.5) / IMG_WIDTH - 1.0).reshape(1, 1, IMG_WIDTH, 1)
    images = (noise + 1.5 * row_amp * row_pos + col_amp * col_pos).astype(jnp.bfloat16)
    return {
        "x": images,
        "w_a": conv_weights(sub_keys[1], (LAYERS_A,), CHAN_A, CHAN_A),
        "bn_a": norm_pairs(sub_keys[2], (LAYERS_A,), CHAN_A),
        "w_down": conv_weights(sub_keys[3], (), CHAN_A, CHAN_B),
        "bn_down": norm_pairs(sub_keys[4], (), CHAN_B),
        "w_b": conv_weights(sub_keys[5], (LAYERS_B,), CHAN_B, CHAN_B),
        "bn_b": norm_pairs(sub_keys[6], (LAYERS_B,), CHAN_B),
    }


def conv_bn(act_in, weight, norm_pair, stride, pad_pairs):
    pre_norm = lax.conv_general_dilated(act_in.astype(jnp.float32), weight.astype(jnp.float32), (stride, stride), pad_pairs, dimension_numbers=CONV_DIMS)
    num_pos = pre_norm.shape[0] * pre_norm.shape[1] * pre_norm.shape[2]
    mean_val = jnp.sum(pre_norm, axis=(0, 1, 2)) / num_pos
    var_val = jnp.sum(pre_norm * pre_norm, axis=(0, 1, 2)) / num_pos - mean_val * mean_val
    normed = norm_pair[0] * (pre_norm - mean_val) * lax.rsqrt(var_val + 1e-5) + norm_pair[1]
    return jnp.maximum(normed, 0.0).astype(jnp.bfloat16)


def reference(x, w_a, bn_a, w_down, bn_down, w_b, bn_b):
    def stage_step(carry_act, layer_in):
        return conv_bn(carry_act, layer_in[0], layer_in[1], 1, SAME_PADS), None

    act_out, scan_rest = lax.scan(stage_step, x, (w_a, bn_a))
    act_out = conv_bn(act_out, w_down, bn_down, 2, DOWN_PADS)
    act_out, scan_rest = lax.scan(stage_step, act_out, (w_b, bn_b))
    return act_out
```

```python
import functools

import jax
import jax.numpy as jnp
from jax import lax
from jax.experimental import pallas as pl
from jax.experimental.pallas import tpu as pltpu
from jax.sharding import PartitionSpec as P

MESH = pl.DeviceIdType.MESH
F32 = jnp.float32
BF16 = jnp.bfloat16
LANES = 128
SUB = 8
EPS = 1e-5
KINDS = ((-1, 0), (1, 0), (0, -1), (0, 1), (-1, -1), (-1, 1), (1, -1), (1, 1))


def stack_kernel(dims, x_hbm, wa_hbm, bna_ref, wd_hbm, bnd_ref, wb_hbm, bnb_ref, out_ref,
                 wsl, xs, xrow, ya, yb, za, zd, zb, rowa, rowb, csa, cra, csb, crb, sta, std, stb, acc, prm,
                 wsem, xsem, xss, xrs, hs, hr, ss, sr):
    n_i, n_j, imgs, rows, cols, chan = dims
    n_dev = n_i * n_j
    cba = chan // LANES
    cbb = 2 * cba
    pa, pb = ya.shape[3], yb.shape[3]
    ma, colb, rowsb = imgs * cols, cols // 2, rows // 2
    mb = imgs * colb
    layers_a = wa_hbm.shape[0]
    i = lax.axis_index("sp")
    j = lax.axis_index("sp2")
    me = i * n_j + j
    core = lax.rem(i, 2)
    row_loc = (rows - 1) * (1 - core)
    row_rem = (rows - 1) * core

    def here(di, dj):
        a, b = i + di, j + dj
        return (a >= 0) & (a < n_i) & (b >= 0) & (b < n_j)

    def w_copies(slot, src):
        return pltpu.make_async_copy(src, wsl.at[slot % 6], wsem.at[slot])

    def wa_copy(l):
        return w_copies(l, wa_hbm.at[l])

    def wd_copy(nh):
        return w_copies(layers_a + nh, wd_hbm.at[:, :, :, pl.ds(nh * chan, chan)])

    def wb_copy(q):
        src = wb_hbm.at[0, :, :, pl.ds((q // 2) * chan, chan), pl.ds((q % 2) * chan, chan)]
        return w_copies(layers_a + 2 + q, src)

    xcopy = pltpu.make_async_copy(x_hbm, xs, xsem)
    xcopy.start()
    for l in range(layers_a):
        wa_copy(l).start()
    for nh in range(2):
        wd_copy(nh).start()

    barrier = pltpu.get_barrier_semaphore()

    def peer(p):
        t = lax.rem(me + p, n_dev)
        return {"sp": t // n_j, "sp2": lax.rem(t, n_j)}

    def greet(p, c):
        pl.semaphore_signal(barrier, inc=1, device_id=peer(p), device_id_type=MESH)
        return c

    lax.fori_loop(1, n_dev, greet, 0)

    def wipe(y):
        def go(t, c):
            y[t] = jnp.zeros(y.shape[1:], F32)
            return c

        lax.fori_loop(0, y.shape[0], go, 0)

    wipe(ya)
    wipe(yb)

    xcopy.wait()
    pl.semaphore_wait(barrier, n_dev - 1)

    def target(k):
        di, dj = KINDS[k]
        return {"sp": i + di, "sp2": j + dj}

    def halo_copy(k, set_, z, row, cs, cr, n_rows):
        di, dj = KINDS[k]
        slot = {-1: n_rows + 1, 1: 0}.get(di)
        edge = 0 if di < 0 else n_rows - 1
        side_here, side_there = (0, 1) if dj < 0 else (1, 0)
        if dj == 0:
            src, dst = z.at[edge], row.at[1 if di < 0 else 0]
        elif di == 0:
            src, dst = cs.at[side_here], cr.at[side_there, pl.ds(1, n_rows)]
        else:
            src, dst = cs.at[side_here, edge], cr.at[side_there, slot]
        return pltpu.make_async_remote_copy(src_ref=src, dst_ref=dst, send_sem=hs.at[set_, k], recv_sem=hr.at[set_, k],
                                            device_id=target(k), device_id_type=MESH)

    def halo_start(k, *args):
        @pl.when(here(*KINDS[k]))
        def _():
            halo_copy(k, *args).start()

    def halo_sent(k, *args):
        @pl.when(here(*KINDS[k]))
        def _():
            halo_copy(k, *args).wait_send()

    def got(k):
        return here(-KINDS[k][0], -KINDS[k][1])

    def xrow_copy(k):
        di = KINDS[k][0]
        return pltpu.make_async_remote_copy(src_ref=xs.at[:, 0 if di < 0 else rows - 1], dst_ref=xrow.at[1 if di < 0 else 0],
                                            send_sem=xss.at[k], recv_sem=xrs.at[k], device_id=target(k), device_id_type=MESH)

    for k in (0, 1):
        @pl.when(here(*KINDS[k]))
        def _():
            xrow_copy(k).start()

    def lines(y):
        return y.reshape(y.shape[0], y.shape[1], y.shape[2] * y.shape[3], LANES)

    def fill_x(s, piece):
        for cb in range(cba):
            ya[s, cb, :, pl.ds(SUB, cols), :] = piece(pl.ds(cb * LANES, LANES)).astype(F32)

    def own_x(r, c):
        fill_x(r + 1, lambda cl: xs[:, r, :, cl])
        for cb in range(cba):
            csa[0, r, cb] = lines(ya)[r + 1, cb, pl.ds(SUB, imgs, stride=pa), :]
            csa[1, r, cb] = lines(ya)[r + 1, cb, pl.ds(SUB + cols - 1, imgs, stride=pa), :]
        return c

    lax.fori_loop(0, rows, own_x, 0)
    args_x = (1, za, None, csa, cra.at[1], rows)
    for k in range(2, 8):
        halo_start(k, *args_x)

    def norm(v, cb):
        mean, rs, gain, shift = (prm[q, pl.ds(cb, 1), :] for q in range(4))
        return jnp.maximum(gain * (v - mean) * rs + shift, 0.0)

    def params(st, n_pos, bn, n_cb):
        tot = st[0]
        for d in range(1, n_dev):
            tot = tot + st[d]
        mean = tot[0:n_cb] / n_pos
        var = tot[n_cb:2 * n_cb] / n_pos - mean * mean
        prm[0, pl.ds(0, n_cb), :] = mean
        prm[1, pl.ds(0, n_cb), :] = lax.rsqrt(var + EPS)
        for cb in range(n_cb):
            cl = pl.ds(cb * LANES, LANES)
            prm[2, pl.ds(cb, 1), :] = bn[pl.ds(0, 1), cl]
            prm[3, pl.ds(cb, 1), :] = bn[pl.ds(1, 1), cl]

    def fill_row(y, s, src, n_cb, pitch, n_col):
        for cb in range(n_cb):
            y[s, cb, :, pl.ds(SUB, n_col), :] = norm(src[cb], cb).reshape(imgs, n_col, LANES)

    def fill_col(y, side, s, cr, n_cb, pitch, n_col, plain):
        at = SUB - 1 if side == 0 else SUB + n_col
        for cb in range(n_cb):
            v = cr[side, s, cb]
            lines(y)[s, cb, pl.ds(at, imgs, stride=pitch), :] = v if plain else norm(v, cb)

    def fill_side_cols(y, set_, z, row, cs, cr, n_rows, n_cb, pitch, n_col, plain):
        for k in (2, 3):
            @pl.when(got(k))
            def _():
                halo_copy(k, set_, z, row, cs, cr, n_rows).wait_recv()
                for s in range(1, n_rows + 1):
                    fill_col(y, 1 if k == 2 else 0, s, cr, n_cb, pitch, n_col, plain)

    def fill_halo_row(y, below, set_, z, row, cs, cr, n_rows, n_cb, pitch, n_col, first):
        args = (set_, z, row, cs, cr, n_rows)
        k = 0 if below else 1
        s = n_rows + 1 if below else 0

        @pl.when(got(k))
        def _():
            if first:
                xrow_copy(k).wait_recv()
                fill_x(s, lambda cl: xrow[1 if below else 0, :, :, cl])
            else:
                halo_copy(k, *args).wait_recv()
                fill_row(y, s, row.at[1 if below else 0], n_cb, pitch, n_col)

        for k, side in ((4, 1), (5, 0)) if below else ((6, 1), (7, 0)):
            @pl.when(got(k))
            def _():
                halo_copy(k, *args).wait_recv()
                fill_col(y, side, s, cr, n_cb, pitch, n_col, first)

    def lhs_of(y, r, n_cb, pitch, starts, n_col, row_step, cb0=0, stride=1, slot0=0):
        parts = []
        for dy in range(3):
            for dx in range(3):
                for cb in range(cb0, cb0 + n_cb):
                    idx = pl.ds(starts + dx, n_col) if stride == 1 else pl.ds(starts + dx, n_col, stride=stride)
                    v = y[row_step * r + slot0 + dy, cb, :, idx, :]
                    parts.append(v.reshape(imgs * n_col, LANES).astype(BF16))
        return jnp.concatenate(parts, axis=1)

    def weights(slot):
        return wsl[slot].reshape(9 * chan, chan)

    def dot(a, b):
        return jnp.dot(a, b, preferred_element_type=F32)

    def add_stats(v, lane0):
        cl = pl.ds(lane0, v.shape[1])
        v3 = v.reshape(v.shape[0] // SUB, SUB, v.shape[1])
        acc[0, :, cl] += jnp.sum(v3, axis=0)
        acc[1, :, cl] += jnp.sum(v3 * v3, axis=0)

    def stat_copy(st, q, p):
        return pltpu.make_async_remote_copy(src_ref=st.at[me], dst_ref=st.at[me], send_sem=ss.at[q], recv_sem=sr.at[q],
                                            device_id=peer(p), device_id_type=MESH)

    def send_stats(st, q, n_cb):
        for m in range(2):
            tot = jnp.sum(acc[m, :, pl.ds(0, n_cb * LANES)], axis=0, keepdims=True)
            for cb in range(n_cb):
                st[me, pl.ds(m * n_cb + cb, 1), :] = tot[:, cb * LANES:(cb + 1) * LANES]

        def go(p, c):
            stat_copy(st, q, p).start()
            return c

        lax.fori_loop(1, n_dev, go, 0)

    def all_of(st, sem):
        part = st.at[pl.ds(0, n_dev - 1)]
        return pltpu.make_async_copy(part, part, sem)

    def clear_stats():
        acc[...] = jnp.zeros_like(acc)

    def mm_row_a(slot, r):
        v = dot(lhs_of(ya, r, cba, pa, SUB - 1, cols, 1), weights(slot))
        add_stats(v, 0)
        for cb in range(cba):
            za[r, cb] = v[:, cb * LANES:(cb + 1) * LANES]

    def layer_a(l, first):
        par = lax.rem(l, 2)
        prev = 1 if first else 1 - par
        args_in = (prev, za, rowa.at[prev], csa, cra.at[prev], rows)
        args_out = (par, za, rowa.at[par], csa, cra.at[par], rows)
        clear_stats()
        if not first:
            def own(r, c):
                fill_row(ya, r + 1, za.at[r], cba, pa, cols)
                return c

            lax.fori_loop(0, rows, own, 0)
        fill_side_cols(ya, *args_in, cba, pa, cols, first)
        wa_copy(l).wait()

        def interior(r, c):
            mm_row_a(l, r)
            return c

        lax.fori_loop(1, rows - 1, interior, 0)

        for k in (0, 1):
            if first:
                @pl.when(here(*KINDS[k]))
                def _():
                    xrow_copy(k).wait_send()
            else:
                halo_sent(k, *args_in)
        for k in range(2, 8):
            halo_sent(k, *args_in)

        for below in (True, False):
            fill_halo_row(ya, below, *args_in, cba, pa, cols, first)

        def edge(t, c):
            mm_row_a(l, jnp.where(t == 0, row_loc, row_rem))
            return c

        lax.fori_loop(0, 2, edge, 0)
        if not first:
            all_of(sta.at[1 - par], ss.at[1 - par]).wait()
        send_stats(sta.at[par], par, cba)
        for side in range(2):
            for r in range(rows):
                for cb in range(cba):
                    csa[side, r, cb] = za[r, cb, pl.ds(side * (cols - 1), imgs, stride=cols), :]
        for k in range(8):
            halo_start(k, *args_out)
        all_of(sta.at[par], sr.at[par]).wait()
        params(sta.at[par], float(n_i * n_j * rows * ma), bna_ref.at[l], cba)

    layer_a(0, True)
    wb_copy(0).start()

    def more(l, c):
        layer_a(l, False)
        return c

    lax.fori_loop(1, layers_a, more, 0)
    for q in range(1, 4):
        wb_copy(q).start()

    last = (layers_a - 1) % 2
    args_in = (last, za, rowa.at[last], csa, cra.at[last], rows)
    args_out = (2, zd, rowb, csb, crb, rowsb)
    clear_stats()

    def own_d(r, c):
        fill_row(ya, r + 1, za.at[r], cba, pa, cols)
        return c

    lax.fori_loop(0, rows, own_d, 0)
    fill_side_cols(ya, *args_in, cba, pa, cols, False)
    for below in (True, False):
        fill_halo_row(ya, below, *args_in, cba, pa, cols, False)
    for k in range(8):
        halo_sent(k, *args_in)
    all_of(sta.at[last], ss.at[last]).wait()
    for nh in range(2):
        wd_copy(nh).wait()

    def down(nh, c):
        a = jnp.concatenate([lhs_of(ya, r, cba, pa, SUB, colb, 2, stride=2, slot0=1) for r in range(rowsb)], axis=0)
        v = dot(a, weights(layers_a + nh))
        v3 = v.reshape(v.shape[0] // SUB, SUB, chan)
        cl = pl.ds(pl.multiple_of(nh * chan, chan), chan)
        acc[0, :, cl] += jnp.sum(v3, axis=0)
        acc[1, :, cl] += jnp.sum(v3 * v3, axis=0)
        for r in range(rowsb):
            for cb in range(cba):
                zd[r, nh * cba + cb] = v[r * mb:(r + 1) * mb, cb * LANES:(cb + 1) * LANES]
        return c

    lax.fori_loop(0, 2, down, 0)
    send_stats(std, 2, cbb)
    for side in range(2):
        for r in range(rowsb):
            for cb in range(cbb):
                csb[side, r, cb] = zd[r, cb, pl.ds(side * (colb - 1), imgs, stride=colb), :]
    for k in range(8):
        halo_start(k, *args_out)
    all_of(std, sr.at[2]).wait()
    n_pos_b = float(n_i * n_j * rowsb * mb)
    params(std, n_pos_b, bnd_ref, cbb)

    clear_stats()

    def own_b(r, c):
        fill_row(yb, r + 1, zd.at[r], cbb, pb, colb)
        return c

    lax.fori_loop(0, rowsb, own_b, 0)
    fill_side_cols(yb, *args_out, cbb, pb, colb, False)
    for below in (True, False):
        fill_halo_row(yb, below, *args_out, cbb, pb, colb, False)
    for q in range(4):
        wb_copy(q).wait()

    def last_mm(nh, c):
        v = None
        for kh in range(2):
            a = jnp.concatenate([lhs_of(yb, r, cba, pb, SUB - 1, colb, 1, cb0=kh * cba) for r in range(rowsb)], axis=0)
            t = dot(a, weights(2 * kh + nh))
            v = t if v is None else v + t
        v3 = v.reshape(v.shape[0] // SUB, SUB, chan)
        cl = pl.ds(pl.multiple_of(nh * chan, chan), chan)
        acc[0, :, cl] += jnp.sum(v3, axis=0)
        acc[1, :, cl] += jnp.sum(v3 * v3, axis=0)
        for r in range(rowsb):
            for cb in range(cba):
                zb[r, nh * cba + cb] = v[r * mb:(r + 1) * mb, cb * LANES:(cb + 1) * LANES]
        return c

    lax.fori_loop(0, 2, last_mm, 0)
    send_stats(stb, 3, cbb)
    for k in range(8):
        halo_sent(k, *args_out)
    all_of(std, ss.at[2]).wait()
    all_of(stb, sr.at[3]).wait()
    params(stb, n_pos_b, bnb_ref.at[0], cbb)

    for r in range(rowsb):
        def fin(g, c):
            at = pl.multiple_of(g * colb, SUB)
            for cb in range(cbb):
                out_ref[g, r, :, pl.ds(cb * LANES, LANES)] = norm(zb[r, cb, pl.ds(at, colb), :], cb).astype(BF16)
            return c

        lax.fori_loop(0, imgs, fin, 0)
    all_of(stb, ss.at[3]).wait()


def solution(mesh):
    n_i, n_j = mesh.shape["sp"], mesh.shape["sp2"]
    n_dev = n_i * n_j

    def per_device(x, w_a, bn_a, w_down, bn_down, w_b, bn_b):
        imgs, rows, cols, chan = x.shape
        chan_b = w_down.shape[-1]
        layers_a = w_a.shape[0]
        cba, cbb = chan // LANES, chan_b // LANES
        colb, rowsb = cols // 2, rows // 2
        ma, mb = imgs * cols, imgs * colb
        pa, pb = cols + 2 * SUB, colb + 2 * SUB
        assert imgs == SUB and layers_a == 4 and w_b.shape[0] == 1 and chan_b == 2 * chan
        dma = pltpu.SemaphoreType.DMA
        hbm = pl.BlockSpec(memory_space=pltpu.HBM)
        vm = pl.BlockSpec(memory_space=pltpu.VMEM)
        scratch = [
            pltpu.VMEM((6, 3, 3, chan, chan), BF16),
            pltpu.VMEM((imgs, rows, cols, chan), BF16),
            pltpu.VMEM((2, imgs, cols, chan), BF16),
            pltpu.VMEM((rows + 2, cba, imgs, pa, LANES), F32),
            pltpu.VMEM((rowsb + 2, cbb, imgs, pb, LANES), F32),
            pltpu.VMEM((rows, cba, ma, LANES), F32),
            pltpu.VMEM((rowsb, cbb, mb, LANES), F32),
            pltpu.VMEM((rowsb, cbb, mb, LANES), F32),
            pltpu.VMEM((2, 2, cba, ma, LANES), F32),
            pltpu.VMEM((2, cbb, mb, LANES), F32),
            pltpu.VMEM((2, rows, cba, SUB, LANES), F32),
            pltpu.VMEM((2, 2, rows + 2, cba, SUB, LANES), F32),
            pltpu.VMEM((2, rowsb, cbb, SUB, LANES), F32),
            pltpu.VMEM((2, rowsb + 2, cbb, SUB, LANES), F32),
            pltpu.VMEM((2, n_dev, 2 * cba, LANES), F32),
            pltpu.VMEM((n_dev, 2 * cbb, LANES), F32),
            pltpu.VMEM((n_dev, 2 * cbb, LANES), F32),
            pltpu.VMEM((2, SUB, chan_b), F32),
            pltpu.VMEM((4, cbb, LANES), F32),
            dma((layers_a + 6,)), dma, dma((2,)), dma((2,)), dma((3, 8)), dma((3, 8)), dma((4,)), dma((4,)),
        ]
        pix = imgs * rows * cols
        flops = 2 * 9 * pix * chan * chan * layers_a + 2 * 9 * (pix // 4) * chan_b * (chan + chan_b)
        return pl.pallas_call(
            functools.partial(stack_kernel, (n_i, n_j, imgs, rows, cols, chan)),
            out_shape=jax.ShapeDtypeStruct((imgs, rowsb, colb, chan_b), BF16),
            in_specs=[hbm, hbm, vm, hbm, vm, hbm, vm],
            out_specs=vm,
            scratch_shapes=scratch,
            cost_estimate=pl.CostEstimate(flops=flops, bytes_accessed=2 * (w_a.size + w_down.size + w_b.size + x.size), transcendentals=0),
            compiler_params=pltpu.CompilerParams(collective_id=0, has_side_effects=True, vmem_limit_bytes=66_000_000),
            name="conv_stack",
        )(x, w_a, bn_a, w_down, bn_down, w_b, bn_b)

    spec = P("dp", "sp", "sp2", None)
    return jax.shard_map(per_device, mesh=mesh, in_specs=(spec, P(), P(), P(), P(), P(), P()), out_specs=spec, check_vma=False)
```

```python
import functools

import jax
import jax.numpy as jnp
from jax import lax
from jax.experimental import pallas as pl
from jax.experimental.pallas import tpu as pltpu
from jax.sharding import PartitionSpec as P

MESH = pl.DeviceIdType.MESH
F32 = jnp.float32
BF16 = jnp.bfloat16
LANES = 128
SUB = 8
EPS = 1e-5
KINDS = ((-1, 0), (1, 0), (0, -1), (0, 1), (-1, -1), (-1, 1), (1, -1), (1, 1))


def stack_kernel(dims, x_hbm, wa_hbm, bna_ref, wd_hbm, bnd_ref, wb_hbm, bnb_ref, out_ref,
                 wsl, xs, xrow, ya, yb, za, zd, zb, rowa, rowb, csa, cra, csb, crb, sta, std, stb, acc, prm,
                 wsem, xsem, xss, xrs, hs, hr, ss, sr):
    n_i, n_j, imgs, rows, cols, chan = dims
    n_dev = n_i * n_j
    half = chan // 2
    nca = half // LANES
    ncb = 2 * nca
    colb, rowsb = cols // 2, rows // 2
    mb = imgs * colb
    ma = imgs * cols
    layers_a = wa_hbm.shape[0]
    i = lax.axis_index("sp")
    j = lax.axis_index("sp2")
    me = i * n_j + j
    core = lax.rem(i, 2)
    chip = i // 2
    n_chip = n_i // 2
    loc_below = core == 0

    moves = [(dx, dc, dy) for dx in range(n_chip) for dc in range(2) for dy in range(n_j)][1:]
    moves.sort(key=lambda t: -(min(t[0], n_chip - t[0]) + min(t[2], n_j - t[2]) + 0.5 * t[1]))
    sp_of = {(dx, dc): lax.rem(chip + dx, n_chip) * 2 + lax.rem(core + dc, 2) for dx in range(n_chip) for dc in range(2)}
    sp2_of = [lax.rem(j + dy, n_j) for dy in range(n_j)]

    def peer(t):
        return {"sp": sp_of[t[0], t[1]], "sp2": sp2_of[t[2]]}

    def here(di, dj):
        a, b = i + di, j + dj
        return (a >= 0) & (a < n_i) & (b >= 0) & (b < n_j)

    def got(k):
        return here(-KINDS[k][0], -KINDS[k][1])

    def target(k):
        return {"sp": i + KINDS[k][0], "sp2": j + KINDS[k][1]}

    def wa_copy(l):
        return pltpu.make_async_copy(wa_hbm.at[l], wsl.at[l], wsem.at[l])

    def wd_copy(nh):
        return pltpu.make_async_copy(wd_hbm.at[:, :, :, pl.ds(nh * chan, chan)], wsl.at[layers_a + nh], wsem.at[layers_a + nh])

    def wb_copy(q):
        at = pl.ds(pl.multiple_of((q // 2) * chan, chan), chan), pl.ds(pl.multiple_of(lax.rem(q, 2) * chan, chan), chan)
        return pltpu.make_async_copy(wb_hbm.at[0, :, :, at[0], at[1]], wsl.at[q], wsem.at[layers_a + 2 + q])

    xcopy = pltpu.make_async_copy(x_hbm, xs, xsem)
    xcopy.start()
    for l in range(layers_a):
        wa_copy(l).start()
    for nh in range(2):
        wd_copy(nh).start()

    barrier = pltpu.get_barrier_semaphore()
    for t in moves:
        pl.semaphore_signal(barrier, inc=1, device_id=peer(t), device_id_type=MESH)

    def wipe(y):
        def go(t, c):
            y[t] = jnp.zeros(y.shape[1:], F32)
            return c

        lax.fori_loop(0, y.shape[0], go, 0)

    wipe(ya)
    xcopy.wait()
    pl.semaphore_wait(barrier, n_dev - 1)

    def halo_copy(k, c, set_, z, row, cs, cr):
        di, dj = KINDS[k]
        n_rows, n_cb = cs.shape[2], cs.shape[3]
        slot = n_rows + 1 if di < 0 else 0
        edge = 0 if di < 0 else n_rows - 1
        side_here, side_there = (0, 1) if dj < 0 else (1, 0)
        if dj == 0:
            src, dst = z.at[edge, pl.ds(c * n_cb, n_cb)], row.at[1 if di < 0 else 0, pl.ds(c * n_cb, n_cb)]
        elif di == 0:
            src, dst = cs.at[c, side_here], cr.at[c, side_there, pl.ds(1, n_rows)]
        else:
            src, dst = cs.at[c, side_here, edge], cr.at[c, side_there, slot]
        return pltpu.make_async_remote_copy(src_ref=src, dst_ref=dst, send_sem=hs.at[set_, c, k], recv_sem=hr.at[set_, c, k],
                                            device_id=target(k), device_id_type=MESH)

    def halo_start(k, c, bufs, live=None):
        @pl.when(here(*KINDS[k]) if live is None else here(*KINDS[k]) & live)
        def _():
            halo_copy(k, c, *bufs).start()

    def halo_sent(k, c, bufs):
        @pl.when(here(*KINDS[k]))
        def _():
            halo_copy(k, c, *bufs).wait_send()

    def stage_cols(z, cs, c, n_col):
        n_cb = cs.shape[3]
        for side in range(2):
            for r in range(cs.shape[2]):
                for b in range(n_cb):
                    cs[c, side, r, b] = z[r, c * n_cb + b, pl.ds(side * (n_col - 1), imgs, stride=n_col), :]

    def xrow_copy(k, c):
        di = KINDS[k][0]
        cl = pl.ds(c * half, half)
        return pltpu.make_async_remote_copy(src_ref=xs.at[:, 0 if di < 0 else rows - 1, :, cl], dst_ref=xrow.at[1 if di < 0 else 0, :, :, cl],
                                            send_sem=xss.at[c, k], recv_sem=xrs.at[c, k], device_id=target(k), device_id_type=MESH)

    for c in range(2):
        for k in (0, 1):
            @pl.when(here(*KINDS[k]))
            def _():
                xrow_copy(k, c).start()

    def lines(y):
        return y.reshape(y.shape[0], y.shape[1], y.shape[2] * y.shape[3], LANES)

    def fill_x(s, piece, blocks):
        for cb in blocks:
            ya[s, cb, :, pl.ds(SUB, cols), :] = piece(pl.ds(cb * LANES, LANES)).astype(F32)

    def own_x(r, carry):
        fill_x(r + 1, lambda cl: xs[:, r, :, cl], range(2 * nca))
        for cb in range(2 * nca):
            for side in range(2):
                csa[cb // nca, side, r, cb % nca] = lines(ya)[r + 1, cb, pl.ds(SUB + side * (cols - 1), imgs, stride=ya.shape[3]), :]
        return carry

    lax.fori_loop(0, rows, own_x, 0)
    for c in range(2):
        for k in range(2, 8):
            halo_start(k, c, (1, za.at[1], rowa.at[1], csa, cra.at[1]))
    wipe(yb)

    def norm(v, cb):
        mean, rs, gain, shift = (prm[q, pl.ds(cb, 1), :] for q in range(4))
        return jnp.maximum(gain * (v - mean) * rs + shift, 0.0)

    def params(st, n_pos, bn, c, n_cb):
        tot = jnp.sum(st[c], axis=0)
        mean = tot[0:n_cb] / n_pos
        var = tot[n_cb:2 * n_cb] / n_pos - mean * mean
        prm[0, pl.ds(c * n_cb, n_cb), :] = mean
        prm[1, pl.ds(c * n_cb, n_cb), :] = lax.rsqrt(var + EPS)
        for cb in range(c * n_cb, (c + 1) * n_cb):
            cl = pl.ds(cb * LANES, LANES)
            prm[2, pl.ds(cb, 1), :] = bn[pl.ds(0, 1), cl]
            prm[3, pl.ds(cb, 1), :] = bn[pl.ds(1, 1), cl]

    def blocks_of(c, n_cb):
        return range(c * n_cb, (c + 1) * n_cb)

    def fill_row(y, s, src, blocks, n_col):
        for cb in blocks:
            y[s, cb, :, pl.ds(SUB, n_col), :] = norm(src[cb], cb).reshape(imgs, n_col, LANES)

    def fill_own(y, z, c, n_cb, n_rows, n_col):
        def go(r, carry):
            fill_row(y, r + 1, z.at[r], blocks_of(c, n_cb), n_col)
            return carry

        lax.fori_loop(0, n_rows, go, 0)

    def fill_col(y, side, s, c, cr, n_col, plain):
        at = SUB - 1 if side == 0 else SUB + n_col
        n_cb = cr.shape[3]
        for b in range(n_cb):
            v = cr[c, side, s, b]
            w = norm(v, c * n_cb + b)
            lines(y)[s, c * n_cb + b, pl.ds(at, imgs, stride=y.shape[3]), :] = w if plain is None else jnp.where(plain, v, w)

    def fill_sides(y, c, bufs, n_col, plain=None, kinds=(2, 3)):
        n_rows = bufs[3].shape[2]
        for k in kinds:
            @pl.when(got(k))
            def _():
                halo_copy(k, c, *bufs).wait_recv()
                for s in range(1, n_rows + 1):
                    fill_col(y, 1 if k == 2 else 0, s, c, bufs[4], n_col, plain)

    def fill_halo_row(y, below, c, bufs, n_col, cond=True, plain=None, corners=(4, 5, 6, 7)):
        k = 0 if below else 1
        n_rows, n_cb = bufs[3].shape[2], bufs[3].shape[3]
        s = n_rows + 1 if below else 0
        blocks = blocks_of(c, n_cb)

        @pl.when(got(k) & cond)
        def _():
            def from_z():
                halo_copy(k, c, *bufs).wait_recv()
                fill_row(y, s, bufs[2].at[1 if below else 0], blocks, n_col)

            if plain is None:
                from_z()
            else:
                @pl.when(plain)
                def _():
                    xrow_copy(k, c).wait_recv()
                    fill_x(s, lambda cl: xrow[1 if below else 0, :, :, cl], blocks)

                pl.when(jnp.logical_not(plain))(from_z)

        for k2, side in ((4, 1), (5, 0)) if below else ((6, 1), (7, 0)):
            if k2 in corners:
                @pl.when(got(k2) & cond)
                def _():
                    halo_copy(k2, c, *bufs).wait_recv()
                    fill_col(y, side, s, c, bufs[4], n_col, plain)

    def fill_halo_of(y, local, c, bufs, n_col, plain=None):
        for below in (True, False):
            fill_halo_row(y, below, c, bufs, n_col, loc_below if below == local else jnp.logical_not(loc_below), plain)

    def lhs_of(y, r, blocks, start, n_col, stride=1):
        parts = []
        for dy in range(3):
            for dx in range(3):
                for cb in blocks:
                    idx = pl.ds(start + dx, n_col) if stride == 1 else pl.ds(start + dx, n_col, stride=stride)
                    parts.append(y[r + dy, cb, :, idx, :].reshape(imgs * n_col, LANES).astype(BF16))
        return jnp.concatenate(parts, axis=1)

    def weights(slot, k0, nk, n0, nn):
        return wsl[slot, :, :, pl.ds(k0, nk), pl.ds(n0, nn)].reshape(9 * nk, nn)

    def dot(a, b):
        return jnp.dot(a, b, preferred_element_type=F32)

    def put_sums(v, u):
        v3 = v.reshape(v.shape[0] // SUB, SUB, v.shape[1])
        cl = pl.ds(0, v.shape[1])
        acc[u, 0, :, cl] = jnp.sum(v3, axis=0)
        acc[u, 1, :, cl] = jnp.sum(v3 * v3, axis=0)

    def send_stats(st, q, c, n_cb, n_u):
        for m in range(2):
            tot = acc[0, m, :, pl.ds(0, n_cb * LANES)]
            for u in range(1, n_u):
                tot = tot + acc[u, m, :, pl.ds(0, n_cb * LANES)]
            tot = jnp.sum(tot, axis=0, keepdims=True)
            for b in range(n_cb):
                st[c, me, pl.ds(m * n_cb + b, 1), :] = tot[:, b * LANES:(b + 1) * LANES]
        for t in moves:
            pltpu.make_async_remote_copy(src_ref=st.at[c, me], dst_ref=st.at[c, me], send_sem=ss.at[q, c], recv_sem=sr.at[q, c],
                                         device_id=peer(t), device_id_type=MESH).start()

    def stats_all(st, c, sem):
        part = st.at[c, pl.ds(0, n_dev - 1)]
        return pltpu.make_async_copy(part, part, sem)

    pair_loc = jnp.where(loc_below, rows // 2, 0)
    pair_rem = rows // 2 - pair_loc
    hrows = rows // 2
    n_pos_a = float(n_i * n_j * rows * ma)
    n_pos_b = float(n_i * n_j * rowsb * mb)

    def pair_lhs(r0, blocks):
        return jnp.concatenate([lhs_of(ya, r0 + t, blocks, SUB - 1, cols) for t in range(hrows)], axis=0)

    def put_z(z, r0, v, cb0, m):
        for t in range(v.shape[0] // m):
            for b in range(v.shape[1] // LANES):
                z[r0 + t, cb0 + b] = v[t * m:(t + 1) * m, b * LANES:(b + 1) * LANES]

    def get_z(z, r0, n_r, cb0, n_cb):
        return jnp.concatenate([jnp.concatenate([z[r0 + t, cb0 + b] for b in range(n_cb)], axis=1) for t in range(n_r)], axis=0)

    def layer_a(l, carry):
        par = lax.rem(l, 2)
        prev = 1 - par
        first = l == 0
        later = l > 0
        live = l < layers_a - 1
        bin_ = (prev, za.at[prev], rowa.at[prev], csa, cra.at[prev])
        bout = (par, za.at[par], rowa.at[par], csa, cra.at[par])
        z = za.at[par]

        def arrive(c):
            @pl.when(later)
            def _():
                stats_all(sta.at[prev], c, sr.at[prev, c]).wait()
                params(sta.at[prev], n_pos_a, bna_ref.at[jnp.maximum(l - 1, 0)], c, nca)
                fill_own(ya, za.at[prev], c, nca, rows, cols)
                stats_all(sta.at[prev], c, ss.at[prev, c]).wait()

            fill_sides(ya, c, bin_, cols, first)

        def leave(c):
            send_stats(sta.at[par], par, c, nca, 2)
            for k in range(8):
                if k < 2:
                    @pl.when(here(*KINDS[k]) & first)
                    def _():
                        xrow_copy(k, c).wait_send()

                    @pl.when(here(*KINDS[k]) & later)
                    def _():
                        halo_copy(k, c, *bin_).wait_send()
                else:
                    halo_sent(k, c, bin_)
            stage_cols(z, csa, c, cols)
            for k in (2, 3, 4, 5, 6, 7, 0, 1):
                halo_start(k, c, bout, None if k in (0, 2, 4) else live)

        arrive(0)
        fill_halo_of(ya, True, 0, bin_, cols, first)
        wa_copy(l).wait()
        put_z(z, pair_loc, dot(pair_lhs(pair_loc, range(nca)), weights(l, 0, half, 0, chan)), 0, ma)
        fill_halo_of(ya, False, 0, bin_, cols, first)
        put_z(z, pair_rem, dot(pair_lhs(pair_rem, range(nca)), weights(l, 0, half, 0, half)), 0, ma)
        arrive(1)
        fill_halo_of(ya, True, 1, bin_, cols, first)

        def second(u, c):
            @pl.when(u == 1)
            def _():
                fill_halo_of(ya, False, 1, bin_, cols, first)

            r0 = jnp.where(u == 0, pair_loc, pair_rem)
            v = dot(pair_lhs(r0, range(nca, 2 * nca)), weights(l, half, half, 0, half)) + get_z(z, r0, hrows, 0, nca)
            put_sums(v, u)
            put_z(z, r0, v, 0, ma)
            return c

        lax.fori_loop(0, 2, second, 0)
        leave(0)
        v = dot(pair_lhs(pair_rem, range(nca)), weights(l, 0, half, half, half))
        v = v + dot(pair_lhs(pair_rem, range(nca, 2 * nca)), weights(l, half, half, half, half))
        put_sums(v, 0)
        put_z(z, pair_rem, v, nca, ma)
        v = dot(pair_lhs(pair_loc, range(nca, 2 * nca)), weights(l, half, half, half, half)) + get_z(z, pair_loc, hrows, nca, nca)
        put_sums(v, 1)
        put_z(z, pair_loc, v, nca, ma)
        leave(1)
        wb_copy(l).start()
        return carry

    lax.fori_loop(0, layers_a, layer_a, 0)

    last = (layers_a - 1) % 2
    bin_ = (last, za.at[last], rowa.at[last], csa, cra.at[last])
    bmid = (2, zd, rowb, csb, crb)

    def arrive_d(c):
        stats_all(sta.at[last], c, sr.at[last, c]).wait()
        params(sta.at[last], n_pos_a, bna_ref.at[layers_a - 1], c, nca)
        fill_own(ya, za.at[last], c, nca, rows, cols)
        fill_sides(ya, c, bin_, cols, kinds=(2,))
        fill_halo_row(ya, True, c, bin_, cols, corners=(4,))
        stats_all(sta.at[last], c, ss.at[last, c]).wait()
        for k in (0, 2, 4):
            halo_sent(k, c, bin_)

    def leave_d(c):
        send_stats(std, 2, c, ncb, 1)
        stage_cols(zd, csb, c, colb)
        for k in (2, 3, 4, 5, 6, 7, 0, 1):
            halo_start(k, c, bmid)

    def down_lhs(c):
        return jnp.concatenate([lhs_of(ya, 2 * r + 1, blocks_of(c, nca), SUB, colb, 2) for r in range(rowsb)], axis=0)

    arrive_d(0)
    for nh in range(2):
        wd_copy(nh).wait()

    def down0(nh, c):
        v = dot(down_lhs(0), weights(layers_a + nh, 0, half, 0, chan))
        put_z(zd, 0, v, nh * ncb, mb)
        return c

    lax.fori_loop(0, 2, down0, 0)
    arrive_d(1)

    def down1(nh, c):
        v = dot(down_lhs(1), weights(layers_a + nh, half, half, 0, chan)) + get_z(zd, 0, rowsb, nh * ncb, ncb)
        put_sums(v, 0)
        put_z(zd, 0, v, nh * ncb, mb)
        for h in range(2):
            @pl.when(nh == h)
            def _():
                leave_d(h)
        return c

    lax.fori_loop(0, 2, down1, 0)

    def arrive_b(c):
        stats_all(std, c, sr.at[2, c]).wait()
        params(std, n_pos_b, bnd_ref, c, ncb)
        fill_own(yb, zd, c, ncb, rowsb, colb)
        fill_sides(yb, c, bmid, colb)

    row_loc = jnp.where(loc_below, rowsb - 1, 0)

    def row_of(u):
        return jnp.where(u == 0, row_loc, rowsb - 1 - row_loc)

    def b_dot(r, kh, nh):
        return dot(lhs_of(yb, r, blocks_of(kh, ncb), SUB - 1, colb), weights(2 * kh + nh, 0, chan, 0, chan))

    arrive_b(0)
    fill_halo_of(yb, True, 0, bmid, colb)
    for q in range(4):
        wb_copy(q).wait()

    def last0(t, c):
        u, nh = t // 2, lax.rem(t, 2)

        @pl.when(t == 2)
        def _():
            fill_halo_of(yb, False, 0, bmid, colb)

        put_z(zb, row_of(u), b_dot(row_of(u), 0, nh), nh * ncb, mb)
        return c

    lax.fori_loop(0, 4, last0, 0)
    arrive_b(1)
    fill_halo_of(yb, True, 1, bmid, colb)

    def last1(t, c):
        nh, u = t // 2, lax.rem(t, 2)

        @pl.when(t == 1)
        def _():
            fill_halo_of(yb, False, 1, bmid, colb)

        v = b_dot(row_of(u), 1, nh) + get_z(zb, row_of(u), 1, nh * ncb, ncb)
        put_sums(v, u)
        put_z(zb, row_of(u), v, nh * ncb, mb)
        for h in range(2):
            @pl.when(t == 2 * h + 1)
            def _():
                send_stats(stb, 3, h, ncb, 2)
        return c

    lax.fori_loop(0, 4, last1, 0)
    for c in range(2):
        for k in range(8):
            halo_sent(k, c, bmid)
        stats_all(std, c, ss.at[2, c]).wait()

    for c in range(2):
        stats_all(stb, c, sr.at[3, c]).wait()
        params(stb, n_pos_b, bnb_ref.at[0], c, ncb)
        for r in range(rowsb):
            for cb in blocks_of(c, ncb):
                out_ref[:, r, :, pl.ds(cb * LANES, LANES)] = norm(zb[r, cb], cb).reshape(imgs, colb, LANES).astype(BF16)
        stats_all(stb, c, ss.at[3, c]).wait()


def solution(mesh):
    n_i, n_j = mesh.shape["sp"], mesh.shape["sp2"]
    n_dev = n_i * n_j

    def per_device(x, w_a, bn_a, w_down, bn_down, w_b, bn_b):
        imgs, rows, cols, chan = x.shape
        chan_b = w_down.shape[-1]
        layers_a = w_a.shape[0]
        cba, cbb = chan // LANES, chan_b // LANES
        colb, rowsb = cols // 2, rows // 2
        ma, mb = imgs * cols, imgs * colb
        pa, pb = cols + 2 * SUB, colb + 2 * SUB
        assert imgs == SUB and layers_a == 4 and w_b.shape[0] == 1 and chan_b == 2 * chan
        dma = pltpu.SemaphoreType.DMA
        hbm = pl.BlockSpec(memory_space=pltpu.HBM)
        vm = pl.BlockSpec(memory_space=pltpu.VMEM)
        nca, ncb = cba // 2, cbb // 2
        scratch = [
            pltpu.VMEM((layers_a + 2, 3, 3, chan, chan), BF16),
            pltpu.VMEM((imgs, rows, cols, chan), BF16),
            pltpu.VMEM((2, imgs, cols, chan), BF16),
            pltpu.VMEM((rows + 2, cba, imgs, pa, LANES), F32),
            pltpu.VMEM((rowsb + 2, cbb, imgs, pb, LANES), F32),
            pltpu.VMEM((2, rows, cba, ma, LANES), F32),
            pltpu.VMEM((rowsb, cbb, mb, LANES), F32),
            pltpu.VMEM((rowsb, cbb, mb, LANES), F32),
            pltpu.VMEM((2, 2, cba, ma, LANES), F32),
            pltpu.VMEM((2, cbb, mb, LANES), F32),
            pltpu.VMEM((2, 2, rows, nca, SUB, LANES), F32),
            pltpu.VMEM((2, 2, 2, rows + 2, nca, SUB, LANES), F32),
            pltpu.VMEM((2, 2, rowsb, ncb, SUB, LANES), F32),
            pltpu.VMEM((2, 2, rowsb + 2, ncb, SUB, LANES), F32),
            pltpu.VMEM((2, 2, n_dev, 2 * nca, LANES), F32),
            pltpu.VMEM((2, n_dev, 2 * ncb, LANES), F32),
            pltpu.VMEM((2, n_dev, 2 * ncb, LANES), F32),
            pltpu.VMEM((2, 2, SUB, chan), F32),
            pltpu.VMEM((4, cbb, LANES), F32),
            dma((layers_a + 6,)), dma, dma((2, 2)), dma((2, 2)), dma((3, 2, 8)), dma((3, 2, 8)), dma((4, 2)), dma((4, 2)),
        ]
        pix = imgs * rows * cols
        flops = 2 * 9 * pix * chan * chan * layers_a + 2 * 9 * (pix // 4) * chan_b * (chan + chan_b)
        return pl.pallas_call(
            functools.partial(stack_kernel, (n_i, n_j, imgs, rows, cols, chan)),
            out_shape=jax.ShapeDtypeStruct((imgs, rowsb, colb, chan_b), BF16),
            in_specs=[hbm, hbm, vm, hbm, vm, hbm, vm],
            out_specs=vm,
            scratch_shapes=scratch,
            cost_estimate=pl.CostEstimate(flops=flops, bytes_accessed=2 * (w_a.size + w_down.size + w_b.size + x.size), transcendentals=0),
            compiler_params=pltpu.CompilerParams(collective_id=0, has_side_effects=True, vmem_limit_bytes=66_000_000),
            name="conv_stack",
        )(x, w_a, bn_a, w_down, bn_down, w_b, bn_b)

    spec = P("dp", "sp", "sp2", None)
    return jax.shard_map(per_device, mesh=mesh, in_specs=(spec, P(), P(), P(), P(), P(), P()), out_specs=spec, check_vma=False)
```

```python
import functools

import jax
import jax.numpy as jnp
from jax import lax
from jax.experimental import pallas as pl
from jax.experimental.pallas import tpu as pltpu
from jax.sharding import PartitionSpec as P

MESH = pl.DeviceIdType.MESH
F32 = jnp.float32
BF16 = jnp.bfloat16
LANES = 128
SUB = 8
EPS = 1e-5
KINDS = ((-1, 0), (1, 0), (0, -1), (0, 1), (-1, -1), (-1, 1), (1, -1), (1, 1))


def stack_kernel(dims, x_hbm, wa_hbm, bna_ref, wd_hbm, bnd_ref, wb_hbm, bnb_ref, out_ref,
                 wsl, xs, xrow, ya, yb, za, zd, zb, rowa, rowb, csa, cra, csb, crb, sta, std, stb, acc, prm,
                 wsem, xsem, xss, xrs, hs, hr, ss, sr):
    n_i, n_j, imgs, rows, cols, chan = dims
    n_dev = n_i * n_j
    half = chan // 2
    nca = half // LANES
    ncb = 2 * nca
    colb, rowsb = cols // 2, rows // 2
    mb = imgs * colb
    ma = imgs * cols
    layers_a = wa_hbm.shape[0]
    i = lax.axis_index("sp")
    j = lax.axis_index("sp2")
    me = i * n_j + j
    core = lax.rem(i, 2)
    chip = i // 2
    n_chip = n_i // 2
    loc_below = core == 0

    moves = [(dx, dc, dy) for dx in range(n_chip) for dc in range(2) for dy in range(n_j)][1:]
    moves.sort(key=lambda t: -(min(t[0], n_chip - t[0]) + min(t[2], n_j - t[2]) + 0.5 * t[1]))
    sp_of = {(dx, dc): lax.rem(chip + dx, n_chip) * 2 + lax.rem(core + dc, 2) for dx in range(n_chip) for dc in range(2)}
    sp2_of = [lax.rem(j + dy, n_j) for dy in range(n_j)]

    def peer(t):
        return {"sp": sp_of[t[0], t[1]], "sp2": sp2_of[t[2]]}

    def here(di, dj):
        a, b = i + di, j + dj
        return (a >= 0) & (a < n_i) & (b >= 0) & (b < n_j)

    def got(k):
        return here(-KINDS[k][0], -KINDS[k][1])

    def target(k):
        return {"sp": i + KINDS[k][0], "sp2": j + KINDS[k][1]}

    def wa_copy(l):
        return pltpu.make_async_copy(wa_hbm.at[l], wsl.at[l], wsem.at[l])

    def wd_copy(nh):
        return pltpu.make_async_copy(wd_hbm.at[:, :, :, pl.ds(nh * chan, chan)], wsl.at[layers_a + nh], wsem.at[layers_a + nh])

    def wb_copy(q):
        at = pl.ds(pl.multiple_of((q // 2) * chan, chan), chan), pl.ds(pl.multiple_of(lax.rem(q, 2) * chan, chan), chan)
        return pltpu.make_async_copy(wb_hbm.at[0, :, :, at[0], at[1]], wsl.at[q], wsem.at[layers_a + 2 + q])

    xcopy = pltpu.make_async_copy(x_hbm, xs, xsem)
    xcopy.start()
    wa_copy(0).start()

    barrier = pltpu.get_barrier_semaphore()
    for t in moves:
        pl.semaphore_signal(barrier, inc=1, device_id=peer(t), device_id_type=MESH)

    def wipe(y):
        def go(t, c):
            y[t] = jnp.zeros(y.shape[1:], F32)
            return c

        lax.fori_loop(0, y.shape[0], go, 0)

    wipe(ya)
    xcopy.wait()
    for l in range(1, layers_a):
        wa_copy(l).start()
    for nh in range(2):
        wd_copy(nh).start()
    pl.semaphore_wait(barrier, n_dev - 1)

    def halo_copy(k, c, set_, z, row, cs, cr):
        di, dj = KINDS[k]
        n_rows, n_cb = cs.shape[2], cs.shape[3]
        slot = n_rows + 1 if di < 0 else 0
        edge = 0 if di < 0 else n_rows - 1
        side_here, side_there = (0, 1) if dj < 0 else (1, 0)
        if dj == 0:
            src, dst = z.at[edge, pl.ds(c * n_cb, n_cb)], row.at[1 if di < 0 else 0, pl.ds(c * n_cb, n_cb)]
        elif di == 0:
            src, dst = cs.at[c, side_here], cr.at[c, side_there, pl.ds(1, n_rows)]
        else:
            src, dst = cs.at[c, side_here, edge], cr.at[c, side_there, slot]
        return pltpu.make_async_remote_copy(src_ref=src, dst_ref=dst, send_sem=hs.at[set_, c, k], recv_sem=hr.at[set_, c, k],
                                            device_id=target(k), device_id_type=MESH)

    def halo_start(k, c, bufs, live=None):
        @pl.when(here(*KINDS[k]) if live is None else here(*KINDS[k]) & live)
        def _():
            halo_copy(k, c, *bufs).start()

    def halo_sent(k, c, bufs):
        @pl.when(here(*KINDS[k]))
        def _():
            halo_copy(k, c, *bufs).wait_send()

    def stage_cols(z, cs, c, n_col):
        n_cb = cs.shape[3]
        for side in range(2):
            for r in range(cs.shape[2]):
                for b in range(n_cb):
                    cs[c, side, r, b] = z[r, c * n_cb + b, pl.ds(side * (n_col - 1), imgs, stride=n_col), :]

    def xrow_copy(k, c):
        di = KINDS[k][0]
        cl = pl.ds(c * half, half)
        return pltpu.make_async_remote_copy(src_ref=xs.at[:, 0 if di < 0 else rows - 1, :, cl], dst_ref=xrow.at[1 if di < 0 else 0, :, :, cl],
                                            send_sem=xss.at[c, k], recv_sem=xrs.at[c, k], device_id=target(k), device_id_type=MESH)

    for c in range(2):
        for k in (0, 1):
            @pl.when(here(*KINDS[k]))
            def _():
                xrow_copy(k, c).start()

    def lines(y):
        return y.reshape(y.shape[0], y.shape[1], y.shape[2] * y.shape[3], LANES)

    def fill_x(s, piece, blocks):
        for cb in blocks:
            ya[s, cb, :, pl.ds(SUB, cols), :] = piece(pl.ds(cb * LANES, LANES)).astype(F32)

    def own_x(r, carry):
        fill_x(r + 1, lambda cl: xs[:, r, :, cl], range(2 * nca))
        for cb in range(2 * nca):
            for side in range(2):
                csa[cb // nca, side, r, cb % nca] = lines(ya)[r + 1, cb, pl.ds(SUB + side * (cols - 1), imgs, stride=ya.shape[3]), :]
        return carry

    lax.fori_loop(0, rows, own_x, 0)
    for c in range(2):
        for k in range(2, 8):
            halo_start(k, c, (1, za.at[1], rowa.at[1], csa, cra.at[1]))
    wipe(yb)

    def norm(v, cb):
        mean, rs, gain, shift = (prm[q, pl.ds(cb, 1), :] for q in range(4))
        return jnp.maximum(gain * (v - mean) * rs + shift, 0.0)

    def params(st, n_pos, bn, c, n_cb):
        tot = jnp.sum(st[c], axis=0)
        mean = tot[0:n_cb] / n_pos
        var = tot[n_cb:2 * n_cb] / n_pos - mean * mean
        prm[0, pl.ds(c * n_cb, n_cb), :] = mean
        prm[1, pl.ds(c * n_cb, n_cb), :] = lax.rsqrt(var + EPS)
        for cb in range(c * n_cb, (c + 1) * n_cb):
            cl = pl.ds(cb * LANES, LANES)
            prm[2, pl.ds(cb, 1), :] = bn[pl.ds(0, 1), cl]
            prm[3, pl.ds(cb, 1), :] = bn[pl.ds(1, 1), cl]

    def blocks_of(c, n_cb):
        return range(c * n_cb, (c + 1) * n_cb)

    def fill_row(y, s, src, blocks, n_col):
        for cb in blocks:
            y[s, cb, :, pl.ds(SUB, n_col), :] = norm(src[cb], cb).reshape(imgs, n_col, LANES)

    def fill_own(y, z, c, n_cb, n_rows, n_col):
        def go(r, carry):
            fill_row(y, r + 1, z.at[r], blocks_of(c, n_cb), n_col)
            return carry

        lax.fori_loop(0, n_rows, go, 0)

    def fill_col(y, side, s, c, cr, n_col, plain):
        at = SUB - 1 if side == 0 else SUB + n_col
        n_cb = cr.shape[3]
        for b in range(n_cb):
            v = cr[c, side, s, b]
            w = norm(v, c * n_cb + b)
            lines(y)[s, c * n_cb + b, pl.ds(at, imgs, stride=y.shape[3]), :] = w if plain is None else jnp.where(plain, v, w)

    def fill_sides(y, c, bufs, n_col, plain=None, kinds=(2, 3)):
        n_rows = bufs[3].shape[2]
        for k in kinds:
            @pl.when(got(k))
            def _():
                halo_copy(k, c, *bufs).wait_recv()
                for s in range(1, n_rows + 1):
                    fill_col(y, 1 if k == 2 else 0, s, c, bufs[4], n_col, plain)

    def fill_halo_row(y, below, c, bufs, n_col, cond=True, plain=None, corners=(4, 5, 6, 7)):
        k = 0 if below else 1
        n_rows, n_cb = bufs[3].shape[2], bufs[3].shape[3]
        s = n_rows + 1 if below else 0
        blocks = blocks_of(c, n_cb)

        @pl.when(got(k) & cond)
        def _():
            def from_z():
                halo_copy(k, c, *bufs).wait_recv()
                fill_row(y, s, bufs[2].at[1 if below else 0], blocks, n_col)

            if plain is None:
                from_z()
            else:
                @pl.when(plain)
                def _():
                    xrow_copy(k, c).wait_recv()
                    fill_x(s, lambda cl: xrow[1 if below else 0, :, :, cl], blocks)

                pl.when(jnp.logical_not(plain))(from_z)

        for k2, side in ((4, 1), (5, 0)) if below else ((6, 1), (7, 0)):
            if k2 in corners:
                @pl.when(got(k2) & cond)
                def _():
                    halo_copy(k2, c, *bufs).wait_recv()
                    fill_col(y, side, s, c, bufs[4], n_col, plain)

    def fill_halo_of(y, local, c, bufs, n_col, plain=None):
        for below in (True, False):
            fill_halo_row(y, below, c, bufs, n_col, loc_below if below == local else jnp.logical_not(loc_below), plain)

    def lhs_of(y, r, blocks, start, n_col, stride=1):
        parts = []
        for dy in range(3):
            for dx in range(3):
                for cb in blocks:
                    idx = pl.ds(start + dx, n_col) if stride == 1 else pl.ds(start + dx, n_col, stride=stride)
                    parts.append(y[r + dy, cb, :, idx, :].reshape(imgs * n_col, LANES).astype(BF16))
        return jnp.concatenate(parts, axis=1)

    def weights(slot, k0, nk, n0, nn):
        return wsl[slot, :, :, pl.ds(k0, nk), pl.ds(n0, nn)].reshape(9 * nk, nn)

    def dot(a, b):
        return jnp.dot(a, b, preferred_element_type=F32)

    def put_sums(v, u, more=False):
        v3 = v.reshape(v.shape[0] // SUB, SUB, v.shape[1])
        cl = pl.ds(0, v.shape[1])
        for m, w in enumerate((v3, v3 * v3)):
            tot = jnp.sum(w, axis=0)
            acc[u, m, :, cl] = acc[u, m, :, cl] + tot if more else tot

    def send_stats(st, q, c, n_cb, n_u):
        for m in range(2):
            tot = acc[0, m, :, pl.ds(0, n_cb * LANES)]
            for u in range(1, n_u):
                tot = tot + acc[u, m, :, pl.ds(0, n_cb * LANES)]
            tot = jnp.sum(tot, axis=0, keepdims=True)
            for b in range(n_cb):
                st[c, me, pl.ds(m * n_cb + b, 1), :] = tot[:, b * LANES:(b + 1) * LANES]
        for t in moves:
            pltpu.make_async_remote_copy(src_ref=st.at[c, me], dst_ref=st.at[c, me], send_sem=ss.at[q, c], recv_sem=sr.at[q, c],
                                         device_id=peer(t), device_id_type=MESH).start()

    def stats_all(st, c, sem):
        part = st.at[c, pl.ds(0, n_dev - 1)]
        return pltpu.make_async_copy(part, part, sem)

    pair_loc = jnp.where(loc_below, rows // 2, 0)
    pair_rem = rows // 2 - pair_loc
    hrows = rows // 2
    n_pos_a = float(n_i * n_j * rows * ma)
    n_pos_b = float(n_i * n_j * rowsb * mb)

    def pair_dots(l, r0, k, n):
        w = weights(l, *k, *n)
        blocks = range(k[0] // LANES, (k[0] + k[1]) // LANES)
        return [dot(lhs_of(ya, r0 + t, blocks, SUB - 1, cols), w) for t in range(hrows)]

    def put_z(z, r0, v, cb0, m):
        for t in range(v.shape[0] // m):
            for b in range(v.shape[1] // LANES):
                z[r0 + t, cb0 + b] = v[t * m:(t + 1) * m, b * LANES:(b + 1) * LANES]

    def get_z(z, r0, n_r, cb0, n_cb):
        return jnp.concatenate([jnp.concatenate([z[r0 + t, cb0 + b] for b in range(n_cb)], axis=1) for t in range(n_r)], axis=0)

    def layer_a(l, carry):
        par = lax.rem(l, 2)
        prev = 1 - par
        first = l == 0
        later = l > 0
        live = l < layers_a - 1
        bin_ = (prev, za.at[prev], rowa.at[prev], csa, cra.at[prev])
        bout = (par, za.at[par], rowa.at[par], csa, cra.at[par])
        z = za.at[par]

        def arrive(c):
            @pl.when(later)
            def _():
                stats_all(sta.at[prev], c, sr.at[prev, c]).wait()
                params(sta.at[prev], n_pos_a, bna_ref.at[jnp.maximum(l - 1, 0)], c, nca)
                fill_own(ya, za.at[prev], c, nca, rows, cols)
                stats_all(sta.at[prev], c, ss.at[prev, c]).wait()

            fill_sides(ya, c, bin_, cols, first)

        def leave(c):
            send_stats(sta.at[par], par, c, nca, 2)
            for k in range(8):
                if k < 2:
                    @pl.when(here(*KINDS[k]) & first)
                    def _():
                        xrow_copy(k, c).wait_send()

                    @pl.when(here(*KINDS[k]) & later)
                    def _():
                        halo_copy(k, c, *bin_).wait_send()
                else:
                    halo_sent(k, c, bin_)
            stage_cols(z, csa, c, cols)
            for k in (2, 3, 4, 5, 6, 7, 0, 1):
                halo_start(k, c, bout, None if k in (0, 2, 4) else live)

        lo, hi, full = (0, half), (half, half), (0, chan)

        def finish(u, r0, vs, n):
            cb0 = n[0] // LANES
            for t, v in enumerate(vs):
                put_sums(v, u, t > 0)
                put_z(z, r0 + t, v, cb0, ma)

        def add_z(vs, r0, n):
            return [v + get_z(z, r0 + t, 1, n[0] // LANES, nca) for t, v in enumerate(vs)]

        arrive(0)
        fill_halo_of(ya, True, 0, bin_, cols, first)
        wa_copy(l).wait()
        for t, v in enumerate(pair_dots(l, pair_loc, lo, full)):
            put_z(z, pair_loc + t, v, 0, ma)
        fill_halo_of(ya, False, 0, bin_, cols, first)
        for t, v in enumerate(pair_dots(l, pair_rem, lo, lo)):
            put_z(z, pair_rem + t, v, 0, ma)
        arrive(1)
        fill_halo_of(ya, True, 1, bin_, cols, first)

        def second(u, c):
            @pl.when(u == 1)
            def _():
                fill_halo_of(ya, False, 1, bin_, cols, first)

            r0 = jnp.where(u == 0, pair_loc, pair_rem)
            finish(u, r0, add_z(pair_dots(l, r0, hi, lo), r0, lo), lo)
            return c

        lax.fori_loop(0, 2, second, 0)
        leave(0)
        finish(0, pair_rem, pair_dots(l, pair_rem, full, hi), hi)
        finish(1, pair_loc, add_z(pair_dots(l, pair_loc, hi, hi), pair_loc, hi), hi)
        leave(1)
        wb_copy(l).start()
        return carry

    lax.fori_loop(0, layers_a, layer_a, 0)

    last = (layers_a - 1) % 2
    bin_ = (last, za.at[last], rowa.at[last], csa, cra.at[last])
    bmid = (2, zd, rowb, csb, crb)

    def arrive_d(c):
        stats_all(sta.at[last], c, sr.at[last, c]).wait()
        params(sta.at[last], n_pos_a, bna_ref.at[layers_a - 1], c, nca)
        fill_own(ya, za.at[last], c, nca, rows, cols)
        fill_sides(ya, c, bin_, cols, kinds=(2,))
        fill_halo_row(ya, True, c, bin_, cols, corners=(4,))
        stats_all(sta.at[last], c, ss.at[last, c]).wait()
        for k in (0, 2, 4):
            halo_sent(k, c, bin_)

    def leave_d(c):
        send_stats(std, 2, c, ncb, 1)
        stage_cols(zd, csb, c, colb)
        for k in (2, 3, 4, 5, 6, 7, 0, 1):
            halo_start(k, c, bmid)

    def down_lhs(c):
        return jnp.concatenate([lhs_of(ya, 2 * r + 1, blocks_of(c, nca), SUB, colb, 2) for r in range(rowsb)], axis=0)

    arrive_d(0)
    for nh in range(2):
        wd_copy(nh).wait()

    def down0(nh, c):
        v = dot(down_lhs(0), weights(layers_a + nh, 0, half, 0, chan))
        put_z(zd, 0, v, nh * ncb, mb)
        return c

    lax.fori_loop(0, 2, down0, 0)
    arrive_d(1)

    def down1(nh, c):
        v = dot(down_lhs(1), weights(layers_a + nh, half, half, 0, chan)) + get_z(zd, 0, rowsb, nh * ncb, ncb)
        put_sums(v, 0)
        put_z(zd, 0, v, nh * ncb, mb)
        for h in range(2):
            @pl.when(nh == h)
            def _():
                leave_d(h)
        return c

    lax.fori_loop(0, 2, down1, 0)

    def arrive_b(c):
        stats_all(std, c, sr.at[2, c]).wait()
        params(std, n_pos_b, bnd_ref, c, ncb)
        fill_own(yb, zd, c, ncb, rowsb, colb)
        fill_sides(yb, c, bmid, colb)

    row_loc = jnp.where(loc_below, rowsb - 1, 0)

    def row_of(u):
        return jnp.where(u == 0, row_loc, rowsb - 1 - row_loc)

    def b_dot(r, kh, nh):
        return dot(lhs_of(yb, r, blocks_of(kh, ncb), SUB - 1, colb), weights(2 * kh + nh, 0, chan, 0, chan))

    arrive_b(0)
    fill_halo_of(yb, True, 0, bmid, colb)
    for q in range(4):
        wb_copy(q).wait()

    def last0(t, c):
        u, nh = t // 2, lax.rem(t, 2)

        @pl.when(t == 2)
        def _():
            fill_halo_of(yb, False, 0, bmid, colb)

        put_z(zb, row_of(u), b_dot(row_of(u), 0, nh), nh * ncb, mb)
        return c

    lax.fori_loop(0, 4, last0, 0)
    arrive_b(1)
    fill_halo_of(yb, True, 1, bmid, colb)

    def last1(t, c):
        nh, u = t // 2, lax.rem(t, 2)

        @pl.when(t == 1)
        def _():
            fill_halo_of(yb, False, 1, bmid, colb)

        v = b_dot(row_of(u), 1, nh) + get_z(zb, row_of(u), 1, nh * ncb, ncb)
        put_sums(v, u)
        put_z(zb, row_of(u), v, nh * ncb, mb)
        for h in range(2):
            @pl.when(t == 2 * h + 1)
            def _():
                send_stats(stb, 3, h, ncb, 2)
        return c

    lax.fori_loop(0, 4, last1, 0)
    for c in range(2):
        for k in range(8):
            halo_sent(k, c, bmid)
        stats_all(std, c, ss.at[2, c]).wait()

    for c in range(2):
        stats_all(stb, c, sr.at[3, c]).wait()
        params(stb, n_pos_b, bnb_ref.at[0], c, ncb)
        for r in range(rowsb):
            for cb in blocks_of(c, ncb):
                out_ref[:, r, :, pl.ds(cb * LANES, LANES)] = norm(zb[r, cb], cb).reshape(imgs, colb, LANES).astype(BF16)
        stats_all(stb, c, ss.at[3, c]).wait()


def solution(mesh):
    n_i, n_j = mesh.shape["sp"], mesh.shape["sp2"]
    n_dev = n_i * n_j

    def per_device(x, w_a, bn_a, w_down, bn_down, w_b, bn_b):
        imgs, rows, cols, chan = x.shape
        chan_b = w_down.shape[-1]
        layers_a = w_a.shape[0]
        cba, cbb = chan // LANES, chan_b // LANES
        colb, rowsb = cols // 2, rows // 2
        ma, mb = imgs * cols, imgs * colb
        pa, pb = cols + 2 * SUB, colb + 2 * SUB
        assert imgs == SUB and layers_a == 4 and w_b.shape[0] == 1 and chan_b == 2 * chan
        dma = pltpu.SemaphoreType.DMA
        hbm = pl.BlockSpec(memory_space=pltpu.HBM)
        vm = pl.BlockSpec(memory_space=pltpu.VMEM)
        nca, ncb = cba // 2, cbb // 2
        scratch = [
            pltpu.VMEM((layers_a + 2, 3, 3, chan, chan), BF16),
            pltpu.VMEM((imgs, rows, cols, chan), BF16),
            pltpu.VMEM((2, imgs, cols, chan), BF16),
            pltpu.VMEM((rows + 2, cba, imgs, pa, LANES), F32),
            pltpu.VMEM((rowsb + 2, cbb, imgs, pb, LANES), F32),
            pltpu.VMEM((2, rows, cba, ma, LANES), F32),
            pltpu.VMEM((rowsb, cbb, mb, LANES), F32),
            pltpu.VMEM((rowsb, cbb, mb, LANES), F32),
            pltpu.VMEM((2, 2, cba, ma, LANES), F32),
            pltpu.VMEM((2, cbb, mb, LANES), F32),
            pltpu.VMEM((2, 2, rows, nca, SUB, LANES), F32),
            pltpu.VMEM((2, 2, 2, rows + 2, nca, SUB, LANES), F32),
            pltpu.VMEM((2, 2, rowsb, ncb, SUB, LANES), F32),
            pltpu.VMEM((2, 2, rowsb + 2, ncb, SUB, LANES), F32),
            pltpu.VMEM((2, 2, n_dev, 2 * nca, LANES), F32),
            pltpu.VMEM((2, n_dev, 2 * ncb, LANES), F32),
            pltpu.VMEM((2, n_dev, 2 * ncb, LANES), F32),
            pltpu.VMEM((2, 2, SUB, chan), F32),
            pltpu.VMEM((4, cbb, LANES), F32),
            dma((layers_a + 6,)), dma, dma((2, 2)), dma((2, 2)), dma((3, 2, 8)), dma((3, 2, 8)), dma((4, 2)), dma((4, 2)),
        ]
        pix = imgs * rows * cols
        flops = 2 * 9 * pix * chan * chan * layers_a + 2 * 9 * (pix // 4) * chan_b * (chan + chan_b)
        return pl.pallas_call(
            functools.partial(stack_kernel, (n_i, n_j, imgs, rows, cols, chan)),
            out_shape=jax.ShapeDtypeStruct((imgs, rowsb, colb, chan_b), BF16),
            in_specs=[hbm, hbm, vm, hbm, vm, hbm, vm],
            out_specs=vm,
            scratch_shapes=scratch,
            cost_estimate=pl.CostEstimate(flops=flops, bytes_accessed=2 * (w_a.size + w_down.size + w_b.size + x.size), transcendentals=0),
            compiler_params=pltpu.CompilerParams(collective_id=0, has_side_effects=True, vmem_limit_bytes=66_000_000),
            name="conv_stack",
        )(x, w_a, bn_a, w_down, bn_down, w_b, bn_b)

    spec = P("dp", "sp", "sp2", None)
    return jax.shard_map(per_device, mesh=mesh, in_specs=(spec, P(), P(), P(), P(), P(), P()), out_specs=spec, check_vma=False)
```

```python
import functools

import jax
import jax.numpy as jnp
from jax import lax
from jax.experimental import pallas as pl
from jax.experimental.pallas import tpu as pltpu
from jax.sharding import PartitionSpec as P

MESH = pl.DeviceIdType.MESH
F32 = jnp.float32
BF16 = jnp.bfloat16
LANES = 128
SUB = 8
EPS = 1e-5
KINDS = ((-1, 0), (1, 0), (0, -1), (0, 1), (-1, -1), (-1, 1), (1, -1), (1, 1))


def stack_kernel(dims, x_hbm, wa_hbm, bna_ref, wd_hbm, bnd_ref, wb_hbm, bnb_ref, out_ref,
                 wsl, xs, xrow, ya, yb, za, zd, zb, rowa, rowb, csa, cra, csb, crb, sta, std, stb, acc, prm,
                 wsem, xsem, xss, xrs, hs, hr, ss, sr):
    n_i, n_j, imgs, rows, cols, chan = dims
    n_dev = n_i * n_j
    half = chan // 2
    nca = half // LANES
    ncb = 2 * nca
    colb, rowsb = cols // 2, rows // 2
    mb = imgs * colb
    ma = imgs * cols
    layers_a = wa_hbm.shape[0]
    i = lax.axis_index("sp")
    j = lax.axis_index("sp2")
    me = i * n_j + j
    core = lax.rem(i, 2)
    chip = i // 2
    n_chip = n_i // 2
    loc_below = core == 0

    moves = [(dx, dc, dy) for dx in range(n_chip) for dc in range(2) for dy in range(n_j)][1:]
    moves.sort(key=lambda t: -(min(t[0], n_chip - t[0]) + min(t[2], n_j - t[2]) + 0.5 * t[1]))
    sp_of = {(dx, dc): lax.rem(chip + dx, n_chip) * 2 + lax.rem(core + dc, 2) for dx in range(n_chip) for dc in range(2)}
    sp2_of = [lax.rem(j + dy, n_j) for dy in range(n_j)]

    def peer(t):
        return {"sp": sp_of[t[0], t[1]], "sp2": sp2_of[t[2]]}

    def here(di, dj):
        a, b = i + di, j + dj
        return (a >= 0) & (a < n_i) & (b >= 0) & (b < n_j)

    def got(k):
        return here(-KINDS[k][0], -KINDS[k][1])

    def target(k):
        return {"sp": i + KINDS[k][0], "sp2": j + KINDS[k][1]}

    def wa_copy(l):
        return pltpu.make_async_copy(wa_hbm.at[l], wsl.at[l], wsem.at[l])

    def wd_copy(nh):
        return pltpu.make_async_copy(wd_hbm.at[:, :, :, pl.ds(nh * chan, chan)], wsl.at[layers_a + nh], wsem.at[layers_a + nh])

    def wb_copy(q):
        at = pl.ds(pl.multiple_of((q // 2) * chan, chan), chan), pl.ds(pl.multiple_of(lax.rem(q, 2) * chan, chan), chan)
        return pltpu.make_async_copy(wb_hbm.at[0, :, :, at[0], at[1]], wsl.at[q], wsem.at[layers_a + 2 + q])

    xcopy = pltpu.make_async_copy(x_hbm, xs, xsem)
    xcopy.start()
    wa_copy(0).start()

    barrier = pltpu.get_barrier_semaphore()
    for t in reversed(moves):
        pl.semaphore_signal(barrier, inc=1, device_id=peer(t), device_id_type=MESH)

    def wipe(y):
        def go(t, c):
            y[t] = jnp.zeros(y.shape[1:], F32)
            return c

        lax.fori_loop(0, y.shape[0], go, 0)

    wipe(ya)
    xcopy.wait()
    for l in range(1, layers_a):
        wa_copy(l).start()
    for nh in range(2):
        wd_copy(nh).start()

    def halo_copy(k, c, set_, z, row, cs, cr):
        di, dj = KINDS[k]
        n_rows, n_cb = cs.shape[2], cs.shape[3]
        slot = n_rows + 1 if di < 0 else 0
        edge = 0 if di < 0 else n_rows - 1
        side_here, side_there = (0, 1) if dj < 0 else (1, 0)
        if dj == 0:
            src, dst = z.at[edge, pl.ds(c * n_cb, n_cb)], row.at[1 if di < 0 else 0, pl.ds(c * n_cb, n_cb)]
        elif di == 0:
            src, dst = cs.at[c, side_here], cr.at[c, side_there, pl.ds(1, n_rows)]
        else:
            src, dst = cs.at[c, side_here, edge], cr.at[c, side_there, slot]
        return pltpu.make_async_remote_copy(src_ref=src, dst_ref=dst, send_sem=hs.at[set_, c, k], recv_sem=hr.at[set_, c, k],
                                            device_id=target(k), device_id_type=MESH)

    def rem_start(c, bufs, pieces, live=True):
        set_, z, row = bufs[:3]
        n_rows, n_cb = bufs[3].shape[2], bufs[3].shape[3]
        m = z.shape[2] // 2
        for k in (0, 1):
            @pl.when(here(*KINDS[k]) & (core == k) & (True if k == 0 else live))
            def _():
                for p in pieces:
                    part = lambda ref, at: ref.at[at, c * n_cb + p // 2, pl.ds((p % 2) * m, m)]
                    pltpu.make_async_remote_copy(src_ref=part(z, 0 if k == 0 else n_rows - 1), dst_ref=part(row, 1 - k),
                                                 send_sem=hs.at[set_, c, k], recv_sem=hr.at[set_, c, k],
                                                 device_id=target(k), device_id_type=MESH).start()

    def halo_start(k, c, bufs, live=None):
        @pl.when(here(*KINDS[k]) if live is None else here(*KINDS[k]) & live)
        def _():
            halo_copy(k, c, *bufs).start()

    def halo_sent(k, c, bufs):
        @pl.when(here(*KINDS[k]))
        def _():
            halo_copy(k, c, *bufs).wait_send()

    def stage_cols(z, cs, c, n_col):
        n_cb = cs.shape[3]
        for side in range(2):
            for r in range(cs.shape[2]):
                for b in range(n_cb):
                    cs[c, side, r, b] = z[r, c * n_cb + b, pl.ds(side * (n_col - 1), imgs, stride=n_col), :]

    def xrow_copy(k, c):
        di = KINDS[k][0]
        cl = pl.ds(c * half, half)
        return pltpu.make_async_remote_copy(src_ref=xs.at[:, 0 if di < 0 else rows - 1, :, cl], dst_ref=xrow.at[1 if di < 0 else 0, :, :, cl],
                                            send_sem=xss.at[c, k], recv_sem=xrs.at[c, k], device_id=target(k), device_id_type=MESH)

    def lines(y):
        return y.reshape(y.shape[0], y.shape[1], y.shape[2] * y.shape[3], LANES)

    def fill_x(s, piece, blocks):
        for cb in blocks:
            ya[s, cb, :, pl.ds(SUB, cols), :] = piece(pl.ds(cb * LANES, LANES)).astype(F32)

    def own_x(r, carry):
        fill_x(r + 1, lambda cl: xs[:, r, :, cl], range(2 * nca))
        for cb in range(2 * nca):
            for side in range(2):
                csa[cb // nca, side, r, cb % nca] = lines(ya)[r + 1, cb, pl.ds(SUB + side * (cols - 1), imgs, stride=ya.shape[3]), :]
        return carry

    lax.fori_loop(0, rows, own_x, 0)
    pl.semaphore_wait(barrier, n_dev - 1)
    for c in range(2):
        for k in range(2, 8):
            halo_start(k, c, (1, za.at[1], rowa.at[1], csa, cra.at[1]))
    for c in range(2):
        for k in (0, 1):
            @pl.when(here(*KINDS[k]))
            def _():
                xrow_copy(k, c).start()
    wipe(yb)

    def norm(v, cb):
        mean, gain, shift = (prm[q, pl.ds(cb, 1), :] for q in range(3))
        return jnp.maximum((v - mean) * gain + shift, 0.0)

    def params(st, n_pos, bn, c, n_cb):
        tot = jnp.sum(st[c], axis=0)
        mean = tot[0:n_cb] / n_pos
        var = tot[n_cb:2 * n_cb] / n_pos - mean * mean
        prm[0, pl.ds(c * n_cb, n_cb), :] = mean
        rs = lax.rsqrt(var + EPS)
        for b in range(n_cb):
            cb = c * n_cb + b
            cl = pl.ds(cb * LANES, LANES)
            prm[1, pl.ds(cb, 1), :] = bn[pl.ds(0, 1), cl] * rs[b:b + 1]
            prm[2, pl.ds(cb, 1), :] = bn[pl.ds(1, 1), cl]

    def blocks_of(c, n_cb):
        return range(c * n_cb, (c + 1) * n_cb)

    def fill_row(y, s, src, blocks, n_col):
        for cb in blocks:
            y[s, cb, :, pl.ds(SUB, n_col), :] = norm(src[cb], cb).reshape(imgs, n_col, LANES)

    def fill_own(y, z, c, n_cb, n_rows, n_col):
        def go(r, carry):
            fill_row(y, r + 1, z.at[r], blocks_of(c, n_cb), n_col)
            return carry

        lax.fori_loop(0, n_rows, go, 0)

    def fill_col(y, side, s, c, cr, n_col, plain):
        at = SUB - 1 if side == 0 else SUB + n_col
        n_cb = cr.shape[3]
        for b in range(n_cb):
            v = cr[c, side, s, b]
            w = norm(v, c * n_cb + b)
            lines(y)[s, c * n_cb + b, pl.ds(at, imgs, stride=y.shape[3]), :] = w if plain is None else jnp.where(plain, v, w)

    def fill_sides(y, c, bufs, n_col, plain=None, kinds=(2, 3)):
        n_rows = bufs[3].shape[2]
        for k in kinds:
            @pl.when(got(k))
            def _():
                halo_copy(k, c, *bufs).wait_recv()
                for s in range(1, n_rows + 1):
                    fill_col(y, 1 if k == 2 else 0, s, c, bufs[4], n_col, plain)

    def fill_halo_row(y, below, c, bufs, n_col, cond=True, plain=None, corners=(4, 5, 6, 7)):
        k = 0 if below else 1
        n_rows, n_cb = bufs[3].shape[2], bufs[3].shape[3]
        s = n_rows + 1 if below else 0
        blocks = blocks_of(c, n_cb)

        @pl.when(got(k) & cond)
        def _():
            def from_z():
                halo_copy(k, c, *bufs).wait_recv()
                fill_row(y, s, bufs[2].at[1 if below else 0], blocks, n_col)

            if plain is None:
                from_z()
            else:
                @pl.when(plain)
                def _():
                    xrow_copy(k, c).wait_recv()
                    fill_x(s, lambda cl: xrow[1 if below else 0, :, :, cl], blocks)

                pl.when(jnp.logical_not(plain))(from_z)

        for k2, side in ((4, 1), (5, 0)) if below else ((6, 1), (7, 0)):
            if k2 in corners:
                @pl.when(got(k2) & cond)
                def _():
                    halo_copy(k2, c, *bufs).wait_recv()
                    fill_col(y, side, s, c, bufs[4], n_col, plain)

    def fill_halo_of(y, local, c, bufs, n_col, plain=None):
        for below in (True, False):
            fill_halo_row(y, below, c, bufs, n_col, loc_below if below == local else jnp.logical_not(loc_below), plain)

    def lhs_of(y, r, blocks, start, n_col, stride=1):
        parts = []
        for dy in range(3):
            for dx in range(3):
                for cb in blocks:
                    idx = pl.ds(start + dx, n_col) if stride == 1 else pl.ds(start + dx, n_col, stride=stride)
                    parts.append(y[r + dy, cb, :, idx, :].reshape(imgs * n_col, LANES).astype(BF16))
        return jnp.concatenate(parts, axis=1)

    def weights(slot, k0, nk, n0, nn):
        return wsl[slot, :, :, pl.ds(k0, nk), pl.ds(n0, nn)].reshape(9 * nk, nn)

    def dot(a, b):
        return jnp.dot(a, b, preferred_element_type=F32)

    def put_sums(v, u, more=False):
        v3 = v.reshape(v.shape[0] // SUB, SUB, v.shape[1])
        cl = pl.ds(0, v.shape[1])
        for m, w in enumerate((v3, v3 * v3)):
            tot = jnp.sum(w, axis=0)
            acc[u, m, :, cl] = acc[u, m, :, cl] + tot if more else tot

    def send_stats(st, q, c, n_cb, n_u):
        for m in range(2):
            tot = acc[0, m, :, pl.ds(0, n_cb * LANES)]
            for u in range(1, n_u):
                tot = tot + acc[u, m, :, pl.ds(0, n_cb * LANES)]
            tot = jnp.sum(tot, axis=0, keepdims=True)
            for b in range(n_cb):
                st[c, me, pl.ds(m * n_cb + b, 1), :] = tot[:, b * LANES:(b + 1) * LANES]
        for t in moves:
            pltpu.make_async_remote_copy(src_ref=st.at[c, me], dst_ref=st.at[c, me], send_sem=ss.at[q, c], recv_sem=sr.at[q, c],
                                         device_id=peer(t), device_id_type=MESH).start()

    def stats_all(st, c, sem):
        part = st.at[c, pl.ds(0, n_dev - 1)]
        return pltpu.make_async_copy(part, part, sem)

    pair_loc = jnp.where(loc_below, rows // 2, 0)
    pair_rem = rows // 2 - pair_loc
    hrows = rows // 2
    n_pos_a = float(n_i * n_j * rows * ma)
    n_pos_b = float(n_i * n_j * rowsb * mb)

    def pair_dots(l, r0, k, n):
        w = weights(l, *k, *n)
        blocks = range(k[0] // LANES, (k[0] + k[1]) // LANES)
        return [dot(lhs_of(ya, r0 + t, blocks, SUB - 1, cols), w) for t in range(hrows)]

    def put_z(z, r0, v, cb0, m):
        for t in range(v.shape[0] // m):
            for b in range(v.shape[1] // LANES):
                z[r0 + t, cb0 + b] = v[t * m:(t + 1) * m, b * LANES:(b + 1) * LANES]

    def get_z(z, r0, n_r, cb0, n_cb):
        return jnp.concatenate([jnp.concatenate([z[r0 + t, cb0 + b] for b in range(n_cb)], axis=1) for t in range(n_r)], axis=0)

    def layer_a(l, carry):
        par = lax.rem(l, 2)
        prev = 1 - par
        first = l == 0
        later = l > 0
        live = l < layers_a - 1
        bin_ = (prev, za.at[prev], rowa.at[prev], csa, cra.at[prev])
        bout = (par, za.at[par], rowa.at[par], csa, cra.at[par])
        z = za.at[par]

        def arrive(c):
            @pl.when(later)
            def _():
                stats_all(sta.at[prev], c, sr.at[prev, c]).wait()
                params(sta.at[prev], n_pos_a, bna_ref.at[jnp.maximum(l - 1, 0)], c, nca)
                fill_own(ya, za.at[prev], c, nca, rows, cols)
                stats_all(sta.at[prev], c, ss.at[prev, c]).wait()

            fill_sides(ya, c, bin_, cols, first)

        def leave(c, pieces):
            send_stats(sta.at[par], par, c, nca, 2)
            for k in range(8):
                if k < 2:
                    @pl.when(here(*KINDS[k]) & first)
                    def _():
                        xrow_copy(k, c).wait_send()

                    @pl.when(here(*KINDS[k]) & later)
                    def _():
                        halo_copy(k, c, *bin_).wait_send()
                else:
                    halo_sent(k, c, bin_)
            stage_cols(z, csa, c, cols)
            for k in range(2, 8):
                halo_start(k, c, bout, None if k in (2, 4) else live)
            for k in (0, 1):
                halo_start(k, c, bout, core != k if k == 0 else (core != k) & live)
            rem_start(c, bout, pieces, live)

        lo, hi, full = (0, half), (half, half), (0, chan)

        def finish(u, r0, vs, n):
            cb0 = n[0] // LANES
            for t, v in enumerate(vs):
                put_sums(v, u, t > 0)
                put_z(z, r0 + t, v, cb0, ma)

        def add_z(vs, r0, n):
            return [v + get_z(z, r0 + t, 1, n[0] // LANES, nca) for t, v in enumerate(vs)]

        arrive(0)
        fill_halo_of(ya, True, 0, bin_, cols, first)
        wa_copy(l).wait()
        for t, v in enumerate(pair_dots(l, pair_loc, lo, full)):
            put_z(z, pair_loc + t, v, 0, ma)
        fill_halo_of(ya, False, 0, bin_, cols, first)
        for t, v in enumerate(pair_dots(l, pair_rem, lo, lo)):
            put_z(z, pair_rem + t, v, 0, ma)
        arrive(1)
        fill_halo_of(ya, True, 1, bin_, cols, first)
        fill_halo_of(ya, False, 1, bin_, cols, first)

        def second(u, c):
            r0 = jnp.where(u == 0, pair_rem, pair_loc)
            finish(u, r0, add_z(pair_dots(l, r0, hi, lo), r0, lo), lo)

            @pl.when(u == 0)
            def _():
                rem_start(0, bout, range(2), live)

            return c

        lax.fori_loop(0, 2, second, 0)
        leave(0, range(2, 4))
        finish(0, pair_rem, pair_dots(l, pair_rem, full, hi), hi)
        rem_start(1, bout, range(1), live)
        finish(1, pair_loc, add_z(pair_dots(l, pair_loc, hi, hi), pair_loc, hi), hi)
        leave(1, range(1, 4))
        wb_copy(l).start()
        return carry

    lax.fori_loop(0, layers_a, layer_a, 0)

    last = (layers_a - 1) % 2
    bin_ = (last, za.at[last], rowa.at[last], csa, cra.at[last])
    bmid = (2, zd, rowb, csb, crb)

    def arrive_d(c):
        stats_all(sta.at[last], c, sr.at[last, c]).wait()
        params(sta.at[last], n_pos_a, bna_ref.at[layers_a - 1], c, nca)
        fill_own(ya, za.at[last], c, nca, rows, cols)
        fill_sides(ya, c, bin_, cols, kinds=(2,))
        fill_halo_row(ya, True, c, bin_, cols, corners=(4,))
        stats_all(sta.at[last], c, ss.at[last, c]).wait()
        for k in (0, 2, 4):
            halo_sent(k, c, bin_)

    def leave_d(c):
        send_stats(std, 2, c, ncb, 1)
        stage_cols(zd, csb, c, colb)
        for k in (2, 3, 4, 5, 6, 7, 0, 1):
            halo_start(k, c, bmid)

    def down_lhs(c):
        return jnp.concatenate([lhs_of(ya, 2 * r + 1, blocks_of(c, nca), SUB, colb, 2) for r in range(rowsb)], axis=0)

    arrive_d(0)
    for nh in range(2):
        wd_copy(nh).wait()

    def down0(nh, c):
        v = dot(down_lhs(0), weights(layers_a + nh, 0, half, 0, chan))
        put_z(zd, 0, v, nh * ncb, mb)
        return c

    lax.fori_loop(0, 2, down0, 0)
    arrive_d(1)

    def down1(nh, c):
        v = dot(down_lhs(1), weights(layers_a + nh, half, half, 0, chan)) + get_z(zd, 0, rowsb, nh * ncb, ncb)
        put_sums(v, 0)
        put_z(zd, 0, v, nh * ncb, mb)
        for h in range(2):
            @pl.when(nh == h)
            def _():
                leave_d(h)
        return c

    lax.fori_loop(0, 2, down1, 0)

    def arrive_b(c):
        stats_all(std, c, sr.at[2, c]).wait()
        params(std, n_pos_b, bnd_ref, c, ncb)
        fill_own(yb, zd, c, ncb, rowsb, colb)
        fill_sides(yb, c, bmid, colb)

    row_loc = jnp.where(loc_below, rowsb - 1, 0)

    def row_of(u):
        return jnp.where(u == 0, row_loc, rowsb - 1 - row_loc)

    def b_dot(r, kh, nh):
        return dot(lhs_of(yb, r, blocks_of(kh, ncb), SUB - 1, colb), weights(2 * kh + nh, 0, chan, 0, chan))

    arrive_b(0)
    fill_halo_of(yb, True, 0, bmid, colb)
    for q in range(4):
        wb_copy(q).wait()

    def last0(t, c):
        u, nh = t // 2, lax.rem(t, 2)

        @pl.when(t == 2)
        def _():
            fill_halo_of(yb, False, 0, bmid, colb)

        put_z(zb, row_of(u), b_dot(row_of(u), 0, nh), nh * ncb, mb)
        return c

    lax.fori_loop(0, 4, last0, 0)
    arrive_b(1)
    fill_halo_of(yb, True, 1, bmid, colb)

    def last1(t, c):
        nh, u = t // 2, lax.rem(t, 2)

        @pl.when(t == 1)
        def _():
            fill_halo_of(yb, False, 1, bmid, colb)

        v = b_dot(row_of(u), 1, nh) + get_z(zb, row_of(u), 1, nh * ncb, ncb)
        put_sums(v, u)
        put_z(zb, row_of(u), v, nh * ncb, mb)
        for h in range(2):
            @pl.when(t == 2 * h + 1)
            def _():
                send_stats(stb, 3, h, ncb, 2)
        return c

    lax.fori_loop(0, 4, last1, 0)
    for c in range(2):
        for k in range(8):
            halo_sent(k, c, bmid)
        stats_all(std, c, ss.at[2, c]).wait()

    for c in range(2):
        stats_all(stb, c, sr.at[3, c]).wait()
        params(stb, n_pos_b, bnb_ref.at[0], c, ncb)
        for r in range(rowsb):
            for cb in blocks_of(c, ncb):
                out_ref[:, r, :, pl.ds(cb * LANES, LANES)] = norm(zb[r, cb], cb).reshape(imgs, colb, LANES).astype(BF16)
        stats_all(stb, c, ss.at[3, c]).wait()


def solution(mesh):
    n_i, n_j = mesh.shape["sp"], mesh.shape["sp2"]
    n_dev = n_i * n_j

    def per_device(x, w_a, bn_a, w_down, bn_down, w_b, bn_b):
        imgs, rows, cols, chan = x.shape
        chan_b = w_down.shape[-1]
        layers_a = w_a.shape[0]
        cba, cbb = chan // LANES, chan_b // LANES
        colb, rowsb = cols // 2, rows // 2
        ma, mb = imgs * cols, imgs * colb
        pa, pb = cols + 2 * SUB, colb + 2 * SUB
        assert imgs == SUB and layers_a == 4 and w_b.shape[0] == 1 and chan_b == 2 * chan
        dma = pltpu.SemaphoreType.DMA
        hbm = pl.BlockSpec(memory_space=pltpu.HBM)
        vm = pl.BlockSpec(memory_space=pltpu.VMEM)
        nca, ncb = cba // 2, cbb // 2
        scratch = [
            pltpu.VMEM((layers_a + 2, 3, 3, chan, chan), BF16),
            pltpu.VMEM((imgs, rows, cols, chan), BF16),
            pltpu.VMEM((2, imgs, cols, chan), BF16),
            pltpu.VMEM((rows + 2, cba, imgs, pa, LANES), F32),
            pltpu.VMEM((rowsb + 2, cbb, imgs, pb, LANES), F32),
            pltpu.VMEM((2, rows, cba, ma, LANES), F32),
            pltpu.VMEM((rowsb, cbb, mb, LANES), F32),
            pltpu.VMEM((rowsb, cbb, mb, LANES), F32),
            pltpu.VMEM((2, 2, cba, ma, LANES), F32),
            pltpu.VMEM((2, cbb, mb, LANES), F32),
            pltpu.VMEM((2, 2, rows, nca, SUB, LANES), F32),
            pltpu.VMEM((2, 2, 2, rows + 2, nca, SUB, LANES), F32),
            pltpu.VMEM((2, 2, rowsb, ncb, SUB, LANES), F32),
            pltpu.VMEM((2, 2, rowsb + 2, ncb, SUB, LANES), F32),
            pltpu.VMEM((2, 2, n_dev, 2 * nca, LANES), F32),
            pltpu.VMEM((2, n_dev, 2 * ncb, LANES), F32),
            pltpu.VMEM((2, n_dev, 2 * ncb, LANES), F32),
            pltpu.VMEM((2, 2, SUB, chan), F32),
            pltpu.VMEM((3, cbb, LANES), F32),
            dma((layers_a + 6,)), dma, dma((2, 2)), dma((2, 2)), dma((3, 2, 8)), dma((3, 2, 8)), dma((4, 2)), dma((4, 2)),
        ]
        pix = imgs * rows * cols
        flops = 2 * 9 * pix * chan * chan * layers_a + 2 * 9 * (pix // 4) * chan_b * (chan + chan_b)
        return pl.pallas_call(
            functools.partial(stack_kernel, (n_i, n_j, imgs, rows, cols, chan)),
            out_shape=jax.ShapeDtypeStruct((imgs, rowsb, colb, chan_b), BF16),
            in_specs=[hbm, hbm, vm, hbm, vm, hbm, vm],
            out_specs=vm,
            scratch_shapes=scratch,
            cost_estimate=pl.CostEstimate(flops=flops, bytes_accessed=2 * (w_a.size + w_down.size + w_b.size + x.size), transcendentals=0),
            compiler_params=pltpu.CompilerParams(collective_id=0, has_side_effects=True, vmem_limit_bytes=66_000_000),
            name="conv_stack",
        )(x, w_a, bn_a, w_down, bn_down, w_b, bn_b)

    spec = P("dp", "sp", "sp2", None)
    return jax.shard_map(per_device, mesh=mesh, in_specs=(spec, P(), P(), P(), P(), P(), P()), out_specs=spec, check_vma=False)
```

```python
import functools

import jax
import jax.numpy as jnp
from jax import lax
from jax.experimental import pallas as pl
from jax.experimental.pallas import tpu as pltpu
from jax.sharding import PartitionSpec as P

MESH = pl.DeviceIdType.MESH
F32 = jnp.float32
BF16 = jnp.bfloat16
LANES = 128
SUB = 8
EPS = 1e-5
KINDS = ((-1, 0), (1, 0), (0, -1), (0, 1), (-1, -1), (-1, 1), (1, -1), (1, 1))


def stack_kernel(dims, x_hbm, wa_hbm, bna_ref, wd_hbm, bnd_ref, wb_hbm, bnb_ref, out_ref,
                 wsl, xs, xrow, ya, yb, za, zd, zb, rowa, rowb, csa, cra, csb, crb, sta, std, stb, acc, prm,
                 wsem, xsem, xss, xrs, hs, hr, ss, sr):
    n_i, n_j, imgs, rows, cols, chan = dims
    n_dev = n_i * n_j
    half = chan // 2
    nca = half // LANES
    ncb = 2 * nca
    colb, rowsb = cols // 2, rows // 2
    mb = imgs * colb
    ma = imgs * cols
    layers_a = wa_hbm.shape[0]
    i = lax.axis_index("sp")
    j = lax.axis_index("sp2")
    me = i * n_j + j
    core = lax.rem(i, 2)
    chip = i // 2
    n_chip = n_i // 2
    loc_below = core == 0

    moves = [(dx, dc, dy) for dx in range(n_chip) for dc in range(2) for dy in range(n_j)][1:]
    moves.sort(key=lambda t: -(min(t[0], n_chip - t[0]) + min(t[2], n_j - t[2]) + 0.5 * t[1]))
    sp_of = {(dx, dc): lax.rem(chip + dx, n_chip) * 2 + lax.rem(core + dc, 2) for dx in range(n_chip) for dc in range(2)}
    sp2_of = [lax.rem(j + dy, n_j) for dy in range(n_j)]

    def peer(t):
        return {"sp": sp_of[t[0], t[1]], "sp2": sp2_of[t[2]]}

    def here(di, dj):
        a, b = i + di, j + dj
        return (a >= 0) & (a < n_i) & (b >= 0) & (b < n_j)

    def got(k):
        return here(-KINDS[k][0], -KINDS[k][1])

    def target(k):
        return {"sp": i + KINDS[k][0], "sp2": j + KINDS[k][1]}

    def wa_copy(l):
        return pltpu.make_async_copy(wa_hbm.at[l], wsl.at[l], wsem.at[l])

    def wd_copy(nh):
        return pltpu.make_async_copy(wd_hbm.at[:, :, :, pl.ds(nh * chan, chan)], wsl.at[layers_a + nh], wsem.at[layers_a + nh])

    def wb_copy(q):
        at = pl.ds(pl.multiple_of((q // 2) * chan, chan), chan), pl.ds(pl.multiple_of(lax.rem(q, 2) * chan, chan), chan)
        return pltpu.make_async_copy(wb_hbm.at[0, :, :, at[0], at[1]], wsl.at[q], wsem.at[layers_a + 2 + q])

    xcopy = pltpu.make_async_copy(x_hbm, xs, xsem)
    xcopy.start()
    wa_copy(0).start()

    barrier = pltpu.get_barrier_semaphore()
    for t in reversed(moves):
        pl.semaphore_signal(barrier, inc=1, device_id=peer(t), device_id_type=MESH)

    def wipe(y):
        def go(t, c):
            y[t] = jnp.zeros(y.shape[1:], F32)
            return c

        lax.fori_loop(0, y.shape[0], go, 0)

    wipe(ya)
    xcopy.wait()
    for l in range(1, layers_a):
        wa_copy(l).start()
    for nh in range(2):
        wd_copy(nh).start()

    def halo_copy(k, c, set_, z, row, cs, cr):
        di, dj = KINDS[k]
        n_rows, n_cb = cs.shape[2], cs.shape[3]
        slot = n_rows + 1 if di < 0 else 0
        edge = 0 if di < 0 else n_rows - 1
        side_here, side_there = (0, 1) if dj < 0 else (1, 0)
        if dj == 0:
            src, dst = z.at[edge, pl.ds(c * n_cb, n_cb)], row.at[1 if di < 0 else 0, pl.ds(c * n_cb, n_cb)]
        elif di == 0:
            src, dst = cs.at[c, side_here], cr.at[c, side_there, pl.ds(1, n_rows)]
        else:
            src, dst = cs.at[c, side_here, edge], cr.at[c, side_there, slot]
        return pltpu.make_async_remote_copy(src_ref=src, dst_ref=dst, send_sem=hs.at[set_, c, k], recv_sem=hr.at[set_, c, k],
                                            device_id=target(k), device_id_type=MESH)

    def rem_start(c, bufs, pieces, live=True):
        set_, z, row = bufs[:3]
        n_rows, n_cb = bufs[3].shape[2], bufs[3].shape[3]
        m = z.shape[2] // 2
        for k in (0, 1):
            @pl.when(here(*KINDS[k]) & (core == k) & (True if k == 0 else live))
            def _():
                for p in pieces:
                    part = lambda ref, at: ref.at[at, c * n_cb + p // 2, pl.ds((p % 2) * m, m)]
                    pltpu.make_async_remote_copy(src_ref=part(z, 0 if k == 0 else n_rows - 1), dst_ref=part(row, 1 - k),
                                                 send_sem=hs.at[set_, c, k], recv_sem=hr.at[set_, c, k],
                                                 device_id=target(k), device_id_type=MESH).start()

    def halo_start(k, c, bufs, live=None):
        @pl.when(here(*KINDS[k]) if live is None else here(*KINDS[k]) & live)
        def _():
            halo_copy(k, c, *bufs).start()

    def halo_sent(k, c, bufs):
        @pl.when(here(*KINDS[k]))
        def _():
            halo_copy(k, c, *bufs).wait_send()

    def stage_cols(z, cs, c, n_col):
        n_cb = cs.shape[3]
        for side in range(2):
            for r in range(cs.shape[2]):
                for b in range(n_cb):
                    cs[c, side, r, b] = z[r, c * n_cb + b, pl.ds(side * (n_col - 1), imgs, stride=n_col), :]

    def xrow_copy(k, c):
        di = KINDS[k][0]
        cl = pl.ds(c * half, half)
        return pltpu.make_async_remote_copy(src_ref=xs.at[:, 0 if di < 0 else rows - 1, :, cl], dst_ref=xrow.at[1 if di < 0 else 0, :, :, cl],
                                            send_sem=xss.at[c, k], recv_sem=xrs.at[c, k], device_id=target(k), device_id_type=MESH)

    def lines(y):
        return y.reshape(y.shape[0], y.shape[1], y.shape[2] * y.shape[3], LANES)

    def fill_x(s, piece, blocks):
        for cb in blocks:
            ya[s, cb, :, pl.ds(SUB, cols), :] = piece(pl.ds(cb * LANES, LANES)).astype(F32)

    def own_x(r, carry):
        fill_x(r + 1, lambda cl: xs[:, r, :, cl], range(2 * nca))
        for cb in range(2 * nca):
            for side in range(2):
                csa[cb // nca, side, r, cb % nca] = lines(ya)[r + 1, cb, pl.ds(SUB + side * (cols - 1), imgs, stride=ya.shape[3]), :]
        return carry

    lax.fori_loop(0, rows, own_x, 0)
    pl.semaphore_wait(barrier, n_dev - 1)
    for c in range(2):
        for k in range(2, 8):
            halo_start(k, c, (1, za.at[1], rowa.at[1], csa, cra.at[1]))
    for c in range(2):
        for k in (0, 1):
            @pl.when(here(*KINDS[k]))
            def _():
                xrow_copy(k, c).start()
    wipe(yb)

    def norm(v, cb):
        mean, gain, shift = (prm[q, pl.ds(cb, 1), :] for q in range(3))
        return jnp.maximum((v - mean) * gain + shift, 0.0)

    def params(st, n_pos, bn, c, n_cb):
        tot = jnp.sum(st[c], axis=0)
        mean = tot[0:n_cb] / n_pos
        var = tot[n_cb:2 * n_cb] / n_pos - mean * mean
        prm[0, pl.ds(c * n_cb, n_cb), :] = mean
        rs = lax.rsqrt(var + EPS)
        for b in range(n_cb):
            cb = c * n_cb + b
            cl = pl.ds(cb * LANES, LANES)
            prm[1, pl.ds(cb, 1), :] = bn[pl.ds(0, 1), cl] * rs[b:b + 1]
            prm[2, pl.ds(cb, 1), :] = bn[pl.ds(1, 1), cl]

    def blocks_of(c, n_cb):
        return range(c * n_cb, (c + 1) * n_cb)

    def fill_row(y, s, src, blocks, n_col):
        for cb in blocks:
            y[s, cb, :, pl.ds(SUB, n_col), :] = norm(src[cb], cb).reshape(imgs, n_col, LANES)

    def fill_own(y, z, c, n_cb, n_rows, n_col):
        def go(r, carry):
            fill_row(y, r + 1, z.at[r], blocks_of(c, n_cb), n_col)
            return carry

        lax.fori_loop(0, n_rows, go, 0)

    def fill_col(y, side, s, c, cr, n_col, plain):
        at = SUB - 1 if side == 0 else SUB + n_col
        n_cb = cr.shape[3]
        for b in range(n_cb):
            v = cr[c, side, s, b]
            w = norm(v, c * n_cb + b)
            lines(y)[s, c * n_cb + b, pl.ds(at, imgs, stride=y.shape[3]), :] = w if plain is None else jnp.where(plain, v, w)

    def fill_sides(y, c, bufs, n_col, plain=None, kinds=(2, 3)):
        n_rows = bufs[3].shape[2]
        for k in kinds:
            @pl.when(got(k))
            def _():
                halo_copy(k, c, *bufs).wait_recv()
                for s in range(1, n_rows + 1):
                    fill_col(y, 1 if k == 2 else 0, s, c, bufs[4], n_col, plain)

    def fill_halo_row(y, below, c, bufs, n_col, cond=True, plain=None, corners=(4, 5, 6, 7)):
        k = 0 if below else 1
        n_rows, n_cb = bufs[3].shape[2], bufs[3].shape[3]
        s = n_rows + 1 if below else 0
        blocks = blocks_of(c, n_cb)

        @pl.when(got(k) & cond)
        def _():
            def from_z():
                halo_copy(k, c, *bufs).wait_recv()
                fill_row(y, s, bufs[2].at[1 if below else 0], blocks, n_col)

            if plain is None:
                from_z()
            else:
                @pl.when(plain)
                def _():
                    xrow_copy(k, c).wait_recv()
                    fill_x(s, lambda cl: xrow[1 if below else 0, :, :, cl], blocks)

                pl.when(jnp.logical_not(plain))(from_z)

        for k2, side in ((4, 1), (5, 0)) if below else ((6, 1), (7, 0)):
            if k2 in corners:
                @pl.when(got(k2) & cond)
                def _():
                    halo_copy(k2, c, *bufs).wait_recv()
                    fill_col(y, side, s, c, bufs[4], n_col, plain)

    def fill_halo_of(y, local, c, bufs, n_col, plain=None):
        for below in (True, False):
            fill_halo_row(y, below, c, bufs, n_col, loc_below if below == local else jnp.logical_not(loc_below), plain)

    def lhs_of(y, r, blocks, start, n_col, stride=1):
        parts = []
        for dy in range(3):
            for dx in range(3):
                for cb in blocks:
                    idx = pl.ds(start + dx, n_col) if stride == 1 else pl.ds(start + dx, n_col, stride=stride)
                    parts.append(y[r + dy, cb, :, idx, :].reshape(imgs * n_col, LANES).astype(BF16))
        return jnp.concatenate(parts, axis=1)

    def weights(slot, k0, nk, n0, nn):
        return wsl[slot, :, :, pl.ds(k0, nk), pl.ds(n0, nn)].reshape(9 * nk, nn)

    def dot(a, b):
        return jnp.dot(a, b, preferred_element_type=F32)

    def put_sums(v, u, more=False, a=0):
        v3 = v.reshape(v.shape[0] // SUB, SUB, v.shape[1])
        cl = pl.ds(0, v.shape[1])
        for m, w in enumerate((v3, v3 * v3)):
            tot = jnp.sum(w, axis=0)
            acc[a, u, m, :, cl] = acc[a, u, m, :, cl] + tot if more else tot

    def send_stats(st, q, c, n_cb, n_u, a=0):
        for m in range(2):
            tot = acc[a, 0, m, :, pl.ds(0, n_cb * LANES)]
            for u in range(1, n_u):
                tot = tot + acc[a, u, m, :, pl.ds(0, n_cb * LANES)]
            tot = jnp.sum(tot, axis=0, keepdims=True)
            for b in range(n_cb):
                st[c, me, pl.ds(m * n_cb + b, 1), :] = tot[:, b * LANES:(b + 1) * LANES]
        for t in moves:
            pltpu.make_async_remote_copy(src_ref=st.at[c, me], dst_ref=st.at[c, me], send_sem=ss.at[q, c], recv_sem=sr.at[q, c],
                                         device_id=peer(t), device_id_type=MESH).start()

    def stats_all(st, c, sem):
        part = st.at[c, pl.ds(0, n_dev - 1)]
        return pltpu.make_async_copy(part, part, sem)

    pair_loc = jnp.where(loc_below, rows // 2, 0)
    pair_rem = rows // 2 - pair_loc
    hrows = rows // 2
    n_pos_a = float(n_i * n_j * rows * ma)
    n_pos_b = float(n_i * n_j * rowsb * mb)

    def pair_dots(l, r0, k, n):
        w = weights(l, *k, *n)
        blocks = range(k[0] // LANES, (k[0] + k[1]) // LANES)
        return [dot(lhs_of(ya, r0 + t, blocks, SUB - 1, cols), w) for t in range(hrows)]

    def put_z(z, r0, v, cb0, m):
        for t in range(v.shape[0] // m):
            for b in range(v.shape[1] // LANES):
                z[r0 + t, cb0 + b] = v[t * m:(t + 1) * m, b * LANES:(b + 1) * LANES]

    def get_z(z, r0, n_r, cb0, n_cb):
        return jnp.concatenate([jnp.concatenate([z[r0 + t, cb0 + b] for b in range(n_cb)], axis=1) for t in range(n_r)], axis=0)

    def layer_a(l, carry):
        par = lax.rem(l, 2)
        prev = 1 - par
        first = l == 0
        later = l > 0
        live = l < layers_a - 1
        bin_ = (prev, za.at[prev], rowa.at[prev], csa, cra.at[prev])
        bout = (par, za.at[par], rowa.at[par], csa, cra.at[par])
        z = za.at[par]

        def arrive(c):
            @pl.when(later)
            def _():
                stats_all(sta.at[prev], c, sr.at[prev, c]).wait()
                params(sta.at[prev], n_pos_a, bna_ref.at[jnp.maximum(l - 1, 0)], c, nca)
                fill_own(ya, za.at[prev], c, nca, rows, cols)
                stats_all(sta.at[prev], c, ss.at[prev, c]).wait()

            fill_sides(ya, c, bin_, cols, first)

        def leave(c, pieces):
            send_stats(sta.at[par], par, c, nca, 2)
            for k in range(8):
                if k < 2:
                    @pl.when(here(*KINDS[k]) & first)
                    def _():
                        xrow_copy(k, c).wait_send()

                    @pl.when(here(*KINDS[k]) & later)
                    def _():
                        halo_copy(k, c, *bin_).wait_send()
                else:
                    halo_sent(k, c, bin_)
            stage_cols(z, csa, c, cols)
            for k in range(2, 8):
                halo_start(k, c, bout, None if k in (2, 4) else live)
            for k in (0, 1):
                halo_start(k, c, bout, core != k if k == 0 else (core != k) & live)
            rem_start(c, bout, pieces, live)

        lo, hi, full = (0, half), (half, half), (0, chan)

        def finish(u, r0, vs, n):
            cb0 = n[0] // LANES
            for t, v in enumerate(vs):
                put_sums(v, u, t > 0)
                put_z(z, r0 + t, v, cb0, ma)

        def add_z(vs, r0, n):
            return [v + get_z(z, r0 + t, 1, n[0] // LANES, nca) for t, v in enumerate(vs)]

        arrive(0)
        fill_halo_of(ya, True, 0, bin_, cols, first)
        wa_copy(l).wait()
        for t, v in enumerate(pair_dots(l, pair_loc, lo, full)):
            put_z(z, pair_loc + t, v, 0, ma)
        fill_halo_of(ya, False, 0, bin_, cols, first)
        for t, v in enumerate(pair_dots(l, pair_rem, lo, lo)):
            put_z(z, pair_rem + t, v, 0, ma)
        arrive(1)
        fill_halo_of(ya, True, 1, bin_, cols, first)
        fill_halo_of(ya, False, 1, bin_, cols, first)

        def second(u, c):
            r0 = jnp.where(u == 0, pair_rem, pair_loc)
            finish(u, r0, add_z(pair_dots(l, r0, hi, lo), r0, lo), lo)

            @pl.when(u == 0)
            def _():
                rem_start(0, bout, range(2), live)

            return c

        lax.fori_loop(0, 2, second, 0)
        leave(0, range(2, 4))
        finish(0, pair_rem, pair_dots(l, pair_rem, full, hi), hi)
        rem_start(1, bout, range(1), live)
        finish(1, pair_loc, add_z(pair_dots(l, pair_loc, hi, hi), pair_loc, hi), hi)
        leave(1, range(1, 4))
        wb_copy(l).start()
        return carry

    lax.fori_loop(0, layers_a, layer_a, 0)

    last = (layers_a - 1) % 2
    bin_ = (last, za.at[last], rowa.at[last], csa, cra.at[last])
    bmid = (2, zd, rowb, csb, crb)

    def arrive_d(c):
        stats_all(sta.at[last], c, sr.at[last, c]).wait()
        params(sta.at[last], n_pos_a, bna_ref.at[layers_a - 1], c, nca)
        fill_own(ya, za.at[last], c, nca, rows, cols)
        fill_sides(ya, c, bin_, cols, kinds=(2,))
        fill_halo_row(ya, True, c, bin_, cols, corners=(4,))
        stats_all(sta.at[last], c, ss.at[last, c]).wait()
        for k in (0, 2, 4):
            halo_sent(k, c, bin_)

    def leave_d(c):
        send_stats(std, 2, c, ncb, 1)
        stage_cols(zd, csb, c, colb)
        for k in (2, 3, 4, 5, 6, 7, 0, 1):
            halo_start(k, c, bmid)

    def down_lhs(c):
        return jnp.concatenate([lhs_of(ya, 2 * r + 1, blocks_of(c, nca), SUB, colb, 2) for r in range(rowsb)], axis=0)

    arrive_d(0)
    for nh in range(2):
        wd_copy(nh).wait()

    def down0(nh, c):
        v = dot(down_lhs(0), weights(layers_a + nh, 0, half, 0, chan))
        put_z(zd, 0, v, nh * ncb, mb)
        return c

    lax.fori_loop(0, 2, down0, 0)
    arrive_d(1)

    def down1(nh, c):
        v = dot(down_lhs(1), weights(layers_a + nh, half, half, 0, chan)) + get_z(zd, 0, rowsb, nh * ncb, ncb)
        put_sums(v, 0)
        put_z(zd, 0, v, nh * ncb, mb)
        for h in range(2):
            @pl.when(nh == h)
            def _():
                leave_d(h)
        return c

    lax.fori_loop(0, 2, down1, 0)

    def arrive_b(c):
        stats_all(std, c, sr.at[2, c]).wait()
        params(std, n_pos_b, bnd_ref, c, ncb)
        fill_own(yb, zd, c, ncb, rowsb, colb)
        fill_sides(yb, c, bmid, colb)

    row_loc = jnp.where(loc_below, rowsb - 1, 0)

    def row_of(u):
        return jnp.where(u == 0, row_loc, rowsb - 1 - row_loc)

    def b_dot(r, kh, nh):
        return dot(lhs_of(yb, r, blocks_of(kh, ncb), SUB - 1, colb), weights(2 * kh + nh, 0, chan, 0, chan))

    arrive_b(0)
    fill_halo_of(yb, True, 0, bmid, colb)
    for q in range(4):
        wb_copy(q).wait()

    def last0(u, c):
        @pl.when(u == 1)
        def _():
            fill_halo_of(yb, False, 0, bmid, colb)

        for nh in range(2):
            put_z(zb, row_of(u), b_dot(row_of(u), 0, nh), nh * ncb, mb)
        return c

    lax.fori_loop(0, 2, last0, 0)
    arrive_b(1)
    fill_halo_of(yb, True, 1, bmid, colb)

    def b_finish(u, nh):
        v = b_dot(row_of(u), 1, nh) + get_z(zb, row_of(u), 1, nh * ncb, ncb)
        put_sums(v, u, a=nh)
        put_z(zb, row_of(u), v, nh * ncb, mb)

    for nh in range(2):
        b_finish(0, nh)
    fill_halo_of(yb, False, 1, bmid, colb)

    def last1(nh, c):
        b_finish(1, nh)
        for h in range(2):
            @pl.when(nh == h)
            def _():
                send_stats(stb, 3, h, ncb, 2, h)
        return c

    lax.fori_loop(0, 2, last1, 0)
    for c in range(2):
        for k in range(8):
            halo_sent(k, c, bmid)
        stats_all(std, c, ss.at[2, c]).wait()

    for c in range(2):
        stats_all(stb, c, sr.at[3, c]).wait()
        params(stb, n_pos_b, bnb_ref.at[0], c, ncb)
        for r in range(rowsb):
            for cb in blocks_of(c, ncb):
                out_ref[:, r, :, pl.ds(cb * LANES, LANES)] = norm(zb[r, cb], cb).reshape(imgs, colb, LANES).astype(BF16)
        stats_all(stb, c, ss.at[3, c]).wait()


def solution(mesh):
    n_i, n_j = mesh.shape["sp"], mesh.shape["sp2"]
    n_dev = n_i * n_j

    def per_device(x, w_a, bn_a, w_down, bn_down, w_b, bn_b):
        imgs, rows, cols, chan = x.shape
        chan_b = w_down.shape[-1]
        layers_a = w_a.shape[0]
        cba, cbb = chan // LANES, chan_b // LANES
        colb, rowsb = cols // 2, rows // 2
        ma, mb = imgs * cols, imgs * colb
        pa, pb = cols + 2 * SUB, colb + 2 * SUB
        assert imgs == SUB and layers_a == 4 and w_b.shape[0] == 1 and chan_b == 2 * chan
        dma = pltpu.SemaphoreType.DMA
        hbm = pl.BlockSpec(memory_space=pltpu.HBM)
        vm = pl.BlockSpec(memory_space=pltpu.VMEM)
        nca, ncb = cba // 2, cbb // 2
        scratch = [
            pltpu.VMEM((layers_a + 2, 3, 3, chan, chan), BF16),
            pltpu.VMEM((imgs, rows, cols, chan), BF16),
            pltpu.VMEM((2, imgs, cols, chan), BF16),
            pltpu.VMEM((rows + 2, cba, imgs, pa, LANES), F32),
            pltpu.VMEM((rowsb + 2, cbb, imgs, pb, LANES), F32),
            pltpu.VMEM((2, rows, cba, ma, LANES), F32),
            pltpu.VMEM((rowsb, cbb, mb, LANES), F32),
            pltpu.VMEM((rowsb, cbb, mb, LANES), F32),
            pltpu.VMEM((2, 2, cba, ma, LANES), F32),
            pltpu.VMEM((2, cbb, mb, LANES), F32),
            pltpu.VMEM((2, 2, rows, nca, SUB, LANES), F32),
            pltpu.VMEM((2, 2, 2, rows + 2, nca, SUB, LANES), F32),
            pltpu.VMEM((2, 2, rowsb, ncb, SUB, LANES), F32),
            pltpu.VMEM((2, 2, rowsb + 2, ncb, SUB, LANES), F32),
            pltpu.VMEM((2, 2, n_dev, 2 * nca, LANES), F32),
            pltpu.VMEM((2, n_dev, 2 * ncb, LANES), F32),
            pltpu.VMEM((2, n_dev, 2 * ncb, LANES), F32),
            pltpu.VMEM((2, 2, 2, SUB, chan), F32),
            pltpu.VMEM((3, cbb, LANES), F32),
            dma((layers_a + 6,)), dma, dma((2, 2)), dma((2, 2)), dma((3, 2, 8)), dma((3, 2, 8)), dma((4, 2)), dma((4, 2)),
        ]
        pix = imgs * rows * cols
        flops = 2 * 9 * pix * chan * chan * layers_a + 2 * 9 * (pix // 4) * chan_b * (chan + chan_b)
        return pl.pallas_call(
            functools.partial(stack_kernel, (n_i, n_j, imgs, rows, cols, chan)),
            out_shape=jax.ShapeDtypeStruct((imgs, rowsb, colb, chan_b), BF16),
            in_specs=[hbm, hbm, vm, hbm, vm, hbm, vm],
            out_specs=vm,
            scratch_shapes=scratch,
            cost_estimate=pl.CostEstimate(flops=flops, bytes_accessed=2 * (w_a.size + w_down.size + w_b.size + x.size), transcendentals=0),
            compiler_params=pltpu.CompilerParams(collective_id=0, has_side_effects=True, vmem_limit_bytes=66_000_000),
            name="conv_stack",
        )(x, w_a, bn_a, w_down, bn_down, w_b, bn_b)

    spec = P("dp", "sp", "sp2", None)
    return jax.shard_map(per_device, mesh=mesh, in_specs=(spec, P(), P(), P(), P(), P(), P()), out_specs=spec, check_vma=False)
```
